512 devices in a mesh: proj: 16 (over z_hi, x, core), scen: 32 (over y, z_lo).
Axes of the slice: x: 4, y: 8, z: 8 (z_hi: 2, z_lo: 4; z = z_hi * 4 + z_lo), core: 2. Of those that a mesh axis runs over, the one named last changes fastest.
Arguments:
- fund_value: float32 [16384, 4096], P('proj', 'scen'), may hold values from 0.5 to 2
- in_force: float32 [16384, 4096], P('proj', 'scen'), may hold values from 0.5 to 1.5
- guarantee_base: float32 [16384, 4096], P('proj', 'scen'), may hold values from 0.5 to 2
- lapse_rate: float32 [16384, 4096], P('proj', 'scen'), may hold values from 0.02 to 0.4
- cohort: int32 [16384], P('proj'), may hold values from 0 to 511, as said below
- product: int32 [16384], P('proj'), may hold values from 0 to 15
- guarantee_type: int32 [16384], P('proj'), may hold values from 0 to 3
- returns: float32 [8, 12, 4096], P(None, None, 'scen'), may hold values from -0.625 to 0.625
- mix_table: float32 [16, 8], replicated, may hold values from 0.05 to 1
- fee_table: float32 [4], replicated, may hold values from 0.001 to 0.01
- rollup_table: float32 [4], replicated, may hold values from 0.01 to 0.08
- fund_vol: float32 [8], replicated, may hold values from 0.15 to 0.6
- closing_sigma_figure: float32 [4096], P('scen'), may hold values from 0.5 to 2
- shocks: float32 [8, 2, 1024], P(None, None, 'scen'), may hold values from -6 to 6
- base_table: float32 [10, 16], replicated, may hold values from 0.03 to 0.2
- year_index: int32 [1], replicated, may hold values from 0 to 9
Outputs:
- fund_next: float32 [16384, 4096], P('proj', 'scen')
- force_next: float32 [16384, 4096], P('proj', 'scen')
- base_next: float32 [16384, 4096], P('proj', 'scen')
- lapse_next: float32 [16384, 4096], P('proj', 'scen')
- benefit_cost_per_account: float32 [512, 4096], P('proj', 'scen')
The draws below stay inside these ranges and needn't reach their ends.
Inputs may be any that keep to these rules, and one draw needn't show every extreme that they name: Each cohort holds exactly 32 model points; the model points of each index of proj include exactly 64 whose cohorts lie in the block of 32 cohorts that any one index of proj owns (cohorts q * 32 onward for index q).
All inputs are finite; a program needn't handle non-finite values.
Results may differ from the reference program's by a relative error of at most 0.00026.
Values sent between devices are 32-bit elements; how exact they have to be, the bound alone decides.
A program may use at most 64 MiB of HBM per device.

```python
import math
import jax
import jax.numpy as jnp
from jax import lax

MP_DEV = 1024
COHORTS = 512
FUNDS = 8
VALUATION_TRIALS = 1024
HORIZON = 2
MONTHS = 12
PRODUCTS = 16
GTYPES = 4
YEARS = 10
MODEL_POINTS = 16384
SCENARIOS = 4096
N_PROJ = 16


def draw_cohort(key, part):
    block = COHORTS // N_PROJ
    share = MP_DEV // N_PROJ
    labels = (jnp.arange(MP_DEV, dtype=jnp.int32) % block).astype(jnp.int32)
    owners = jnp.arange(N_PROJ, dtype=jnp.int32)

    def owner_labels(owner):
        return jax.random.permutation(jax.random.fold_in(key, owner), labels)
    spread_labels = jax.vmap(owner_labels)(owners)
    spread_labels = spread_labels + (owners * block)[:, None]
    placed = spread_labels.reshape(N_PROJ, N_PROJ, share).transpose(1, 0, 2).reshape(N_PROJ, MP_DEV)

    def device_order(device, row):
        return jax.random.permutation(jax.random.fold_in(key, device + 7919), row)
    mixed = jax.vmap(device_order)(owners, placed)
    return mixed.reshape(MODEL_POINTS).astype(jnp.int32)


def with_ends(result, stream_key, low, high):
    dims = result.shape
    spot = [jax.random.randint(jax.random.fold_in(stream_key, axis), (), 0, dims[axis]) for axis in range(len(dims))]
    result = result.at[tuple(spot)].set(low)
    longest = dims.index(max(dims))
    spot[longest] = (spot[longest] + 1) % dims[longest]
    return result.at[tuple(spot)].set(high)


def shard_levels(own_key, shape, cuts, low, high):
    level, own = 1.0, jax.random.fold_in(own_key, 6)
    for axis_at, parts in cuts:
        steps = jnp.exp(jax.random.uniform(jax.random.fold_in(own, axis_at), (parts,), jnp.float32, low / len(cuts), high / len(cuts)))
        level = level * jnp.repeat(steps, shape[axis_at] // parts).reshape([-1 if axis == axis_at else 1 for axis in range(len(shape))])
    return level


def normal_values(key, shape, spread, most, cuts=(), kind=jnp.bfloat16):
    level = shard_levels(key, shape, cuts, -0.22, 0.18) if cuts else 1.0
    values = jax.random.normal(key, shape, jnp.float32) * spread * level
    return jnp.minimum(jnp.maximum(values, -most), most).astype(kind)


def setup_inputs(seed: int = 0) -> dict:
    keys = jax.random.split(jax.random.key(seed), 17)
    fund_value = jnp.clip(jnp.exp(math.log(2.0) - 1.3862944 * jax.random.uniform(keys[0], (MODEL_POINTS, SCENARIOS), jnp.float32) ** shard_levels(keys[0], (MODEL_POINTS, SCENARIOS), ((0, 16), (1, 32)), -0.2, 0.2)), 0.5, 2.0)
    in_force = jnp.clip(0.5 + 1.0 * jax.random.uniform(keys[1], (MODEL_POINTS, SCENARIOS), jnp.float32) ** shard_levels(keys[1], (MODEL_POINTS, SCENARIOS), ((0, 16), (1, 32)), -0.2, 0.2), 0.5, 1.5)
    guarantee_base = jnp.clip(jnp.exp(math.log(2.0) - 1.3862944 * jax.random.uniform(keys[2], (MODEL_POINTS, SCENARIOS), jnp.float32) ** shard_levels(keys[2], (MODEL_POINTS, SCENARIOS), ((0, 16), (1, 32)), -0.2, 0.2)), 0.5, 2.0)
    lapse_rate = jnp.clip(0.02 + 0.38 * jax.random.uniform(keys[3], (MODEL_POINTS, SCENARIOS), jnp.float32) ** shard_levels(keys[3], (MODEL_POINTS, SCENARIOS), ((0, 16), (1, 32)), -0.2, 0.2), 0.02, 0.4)
    cohort = draw_cohort(jax.random.fold_in(keys[16], 71), 0)
    product = with_ends(jax.random.randint(keys[5], (MODEL_POINTS,), 0, PRODUCTS), jax.random.fold_in(keys[5], 1), 0, PRODUCTS - 1).astype(jnp.int32)
    guarantee_type = with_ends(jax.random.randint(keys[6], (MODEL_POINTS,), 0, GTYPES), jax.random.fold_in(keys[6], 1), 0, GTYPES - 1).astype(jnp.int32)
    returns = normal_values(keys[7], (FUNDS, MONTHS, SCENARIOS), 0.04, 0.625, ((2, 32),), jnp.float32)
    mix_table = jnp.clip(jnp.exp(jax.random.uniform(keys[8], (PRODUCTS, FUNDS), jnp.float32, math.log(0.05), math.log(1.0))), 0.05, 1.0)
    fee_table = jnp.clip(jnp.exp(jax.random.uniform(keys[9], (GTYPES,), jnp.float32, math.log(0.001), math.log(0.01))), 0.001, 0.01)
    rollup_table = jnp.clip(jnp.exp(jax.random.uniform(keys[10], (GTYPES,), jnp.float32, math.log(0.01), math.log(0.08))), 0.01, 0.08)
    fund_vol = jnp.clip(jnp.exp(jax.random.uniform(keys[11], (FUNDS,), jnp.float32, math.log(0.15), math.log(0.6))), 0.15, 0.6)
    closing_sigma_figure = jnp.clip(jnp.exp(math.log(2.0) - 1.3862944 * jax.random.uniform(keys[12], (SCENARIOS,), jnp.float32) ** shard_levels(keys[12], (SCENARIOS,), ((0, 32),), -0.2, 0.2)), 0.5, 2.0)
    shocks = normal_values(keys[13], (FUNDS, HORIZON, VALUATION_TRIALS), 1.0, 6.0, ((2, 32),), jnp.float32)
    base_table = jnp.clip(jnp.exp(jax.random.uniform(keys[14], (YEARS, PRODUCTS), jnp.float32, math.log(0.03), math.log(0.2))), 0.03, 0.2)
    year_index = jax.random.randint(keys[15], (1,), 0, YEARS).astype(jnp.int32)
    return dict(fund_value=fund_value, in_force=in_force, guarantee_base=guarantee_base, lapse_rate=lapse_rate, cohort=cohort, product=product, guarantee_type=guarantee_type, returns=returns, mix_table=mix_table, fee_table=fee_table, rollup_table=rollup_table, fund_vol=fund_vol, closing_sigma_figure=closing_sigma_figure, shocks=shocks, base_table=base_table, year_index=year_index)


HIGHEST = lax.Precision.HIGHEST
discount_rate = 0.96
lapse_floor = 0.3
lapse_span = 2.0
lapse_slope = 5.0
lapse_pivot = 0.4


def project(fund_value, in_force, guarantee_base, lapse_rate, mix_rows, fee_rows, rollup_rows, returns):
    keep_fee = (1.0 - fee_rows)[:, None]
    rollup_month = (1.0 + rollup_rows / 12.0)[:, None]
    survive = 1.0 - lapse_rate / 12.0
    for month_step in range(returns.shape[1]):
        growth = 1.0 + jnp.dot(mix_rows, returns[:, month_step, :], precision=HIGHEST, preferred_element_type=jnp.float32)
        fund_value = fund_value * growth * keep_fee
        guarantee_base = jnp.maximum(guarantee_base * rollup_month, fund_value)
        in_force = in_force * survive
    return fund_value, in_force, guarantee_base


def price_rows(scenario_conditions, sigma_figures, embedded_trials):
    factor_count, horizon_count, path_count = embedded_trials.shape
    span_cols = horizon_count * path_count
    flat_paths = embedded_trials.reshape(factor_count, span_cols)
    horizon = jnp.repeat(jnp.arange(1, horizon_count + 1, dtype=jnp.float32), path_count)
    weights = discount_rate ** horizon
    entry_number_overall = scenario_conditions.shape[1]
    target = max(1, (1 << 20) // span_cols)
    block_rows = math.gcd(entry_number_overall, 1 << (target.bit_length() - 1))
    block_count = entry_number_overall // block_rows
    benefit_strike_share = scenario_conditions[0].reshape(block_count, block_rows)
    fund_loads = scenario_conditions[1:]
    distributed_amounts = jnp.sum(fund_loads * fund_loads, axis=0).reshape(block_count, block_rows)
    cohort_sorted_entries = fund_loads.reshape(factor_count, block_count, block_rows).transpose(1, 0, 2)
    sigma_entries = sigma_figures.reshape(block_count, block_rows)

    def valuation_batch(fragment_list):
        money_rows, load_rows, level_part, spread_rows = fragment_list
        shifted = lax.dot_general(flat_paths, load_rows, (((0,), (0,)), ((), ())), precision=HIGHEST, preferred_element_type=jnp.float32)
        exponent = level_part[None, :] * shifted - 0.5 * (level_part * level_part)[None, :] * horizon[:, None] * spread_rows[None, :]
        payoff = jnp.maximum(money_rows[None, :] - jnp.exp(exponent), 0.0)
        return jnp.dot(weights, payoff, precision=HIGHEST)

    valued_amounts = lax.map(valuation_batch, (benefit_strike_share, cohort_sorted_entries, sigma_entries, distributed_amounts))
    return valued_amounts.reshape(entry_number_overall)


def valuation_conditions(scenario_conditions, sigma_figures, embedded_trials):
    cohort_count, columns, scen_count = scenario_conditions.shape
    flat_states = scenario_conditions.transpose(1, 2, 0).reshape(columns, scen_count * cohort_count)
    sigma_entries = jnp.repeat(sigma_figures, cohort_count)
    return price_rows(flat_states, sigma_entries, embedded_trials).reshape(scen_count, cohort_count)


def reference(fund_value, in_force, guarantee_base, lapse_rate, cohort, product, guarantee_type, returns, mix_table, fee_table, rollup_table, fund_vol, closing_sigma_figure, shocks, base_table, year_index):
    mix_norm = mix_table / jnp.sum(mix_table, axis=1, keepdims=True)
    mix_rows = mix_norm[product]
    fee_rows = fee_table[guarantee_type]
    rollup_rows = rollup_table[guarantee_type]
    fund_next, force_next, base_next = project(fund_value, in_force, guarantee_base, lapse_rate, mix_rows, fee_rows, rollup_rows, returns)
    weighted = force_next * fund_next
    value_sum = jax.ops.segment_sum(weighted, cohort, num_segments=COHORTS)
    guarantee_sum = jax.ops.segment_sum(force_next * base_next, cohort, num_segments=COHORTS)
    mix_sums = jnp.stack([jax.ops.segment_sum(weighted * mix_rows[:, factor][:, None], cohort, num_segments=COHORTS) for factor in range(FUNDS)], axis=1)
    scenario_conditions = jnp.concatenate([(guarantee_sum / value_sum)[:, None, :], mix_sums / value_sum[:, None, :] * fund_vol[None, :, None]], axis=1)
    embedded_trials = jnp.cumsum(shocks, axis=1)
    valued_amounts = valuation_conditions(scenario_conditions, closing_sigma_figure, embedded_trials)
    benefit_cost_per_account = valued_amounts.T / VALUATION_TRIALS
    cost_rows = benefit_cost_per_account[cohort]
    base_lapse = base_table[year_index[0]][product]
    lapse_next = base_lapse[:, None] * (lapse_floor + lapse_span * jax.nn.sigmoid(lapse_slope * (lapse_pivot - cost_rows)))
    return fund_next, force_next, base_next, lapse_next, benefit_cost_per_account
```

```python
import functools

import jax
import jax.numpy as jnp
from jax import lax
from jax.experimental import pallas as pl
from jax.experimental.pallas import tpu as pltpu
from jax.sharding import PartitionSpec as P

F32, BF16 = jnp.float32, jnp.bfloat16
MESH = pl.DeviceIdType.MESH
LOG2E = 1.4426950408889634

PLANES, PLANE = 2, 8
RING_Y, RUN_Z = 8, 4
SHARE, BLOCK = 64, 32
ROWS = SHARE + BLOCK + 8
CHUNKS, CHUNK = 4, 8
PART = CHUNK * 8 + CHUNK
KDIM = 32


def split2(x):
    hi = x.astype(BF16).astype(F32)
    return hi, x - hi


def split3(x):
    hi, rest = split2(x)
    mid, lo = split2(rest)
    return hi, mid, lo


def matmul(a, b):
    return jnp.dot(a, b, preferred_element_type=F32)


def rows_of(pieces, lanes):
    row = lax.broadcasted_iota(jnp.int32, (8, lanes), 0)
    out = jnp.zeros((8, lanes), F32)
    for i, piece in enumerate(pieces):
        out = jnp.where(row == i, piece, out)
    return out


def project_kernel(
    blocks,
    fund, force, base, lapse, coh, prod, gtype, ret, mix, fee, roll, table, year,
    fund_o, force_o, base_o, ws_o, ss_o, ri_o,
    fb, ib, bb, lb, wsb, ssb, lm, rm, sem_in, sem_out,
):
    points = fb.shape[0]
    size = points // blocks
    months = ret.shape[0]

    def copies_in(i):
        at = pl.ds(i * size, size)
        return [
            pltpu.make_async_copy(src.at[at], dst.at[at], sem_in.at[i, n])
            for n, (src, dst) in enumerate(((fund, fb), (force, ib), (base, bb), (lapse, lb)))
        ]

    def copies_out(i):
        at = pl.ds(i * size, size)
        return [
            pltpu.make_async_copy(src.at[at], dst.at[at], sem_out.at[i, n])
            for n, (src, dst) in enumerate(
                ((fb, fund_o), (ib, force_o), (bb, base_o), (wsb, ws_o), (ssb, ss_o))
            )
        ]

    for i in range(blocks):
        for c in copies_in(i):
            c.start()

    products = mix.shape[1]
    m = mix[...]
    mix_norm = m / jnp.sum(m, axis=0, keepdims=True)
    prod_row = prod[...]
    hot = jnp.where(
        lax.broadcasted_iota(jnp.int32, (products, points), 0) == prod_row, 1.0, 0.0
    )
    mix_rows = jnp.dot(
        mix_norm, hot, precision=lax.Precision.HIGHEST, preferred_element_type=F32
    )
    g = gtype[...]
    fee_row, roll_row = jnp.zeros(g.shape, F32), jnp.zeros(g.shape, F32)
    for k in range(fee.shape[0]):
        fee_row = jnp.where(g == k, fee[k], fee_row)
        roll_row = jnp.where(g == k, roll[k], roll_row)
    grow = 1.0 + roll_row / 12.0
    kappa = (1.0 - fee_row) / grow
    g2 = grow * grow
    g4 = g2 * g2
    grow_year = g4 * g4 * g4
    a_hi, a_lo = split2(mix_rows * kappa)
    extra = rows_of([*split3(kappa), *split3(grow_year)], points)
    lhs = jnp.concatenate([a_hi, a_hi, a_lo, extra], axis=0)
    lm[...] = lhs.T.astype(BF16)
    row8 = lax.broadcasted_iota(jnp.int32, (8, 128), 0)
    ones = jnp.where(row8 < 3, 1.0, 0.0)
    for t in range(months):
        r_hi, r_lo = split2(ret[t])
        tile = jnp.concatenate([r_hi, r_lo, r_hi, ones], axis=0)
        rm[:, t * 128 : (t + 1) * 128] = tile.astype(BF16)
    last = jnp.where((row8 >= 3) & (row8 < 6), 1.0, 0.0)
    zero = jnp.zeros((8, 128), F32)
    rm[:, months * 128 : (months + 1) * 128] = jnp.concatenate(
        [zero, zero, zero, last], axis=0
    ).astype(BF16)

    owners = points // SHARE
    coh_row = coh[...]
    owner_row = lax.div(coh_row, BLOCK)
    owner_iota = lax.broadcasted_iota(jnp.int32, (owners, points), 0)
    owner_hot = jnp.where(owner_iota == owner_row, 1.0, 0.0)
    before = jnp.where(
        lax.broadcasted_iota(jnp.int32, (128, 128), 0)
        < lax.broadcasted_iota(jnp.int32, (128, 128), 1),
        1.0, 0.0,
    ).astype(BF16)
    offset = lax.broadcasted_iota(jnp.int32, (owners, 1), 0).astype(F32) * float(SHARE)
    places = []
    for b in range(points // 128):
        part = owner_hot[:, b * 128 : (b + 1) * 128]
        rank = matmul(part.astype(BF16), before) + offset
        places.append(jnp.sum(part * rank, axis=0, keepdims=True))
        offset = offset + jnp.sum(part, axis=1, keepdims=True)
    place = jnp.concatenate(places, axis=1)
    lapses = jnp.dot(
        table[...], hot, precision=lax.Precision.HIGHEST, preferred_element_type=F32
    )
    picked = lax.broadcasted_iota(jnp.int32, lapses.shape, 0) == year[0]
    base_lapse = jnp.sum(jnp.where(picked, lapses, 0.0), axis=0, keepdims=True)
    local = coh_row - owner_row * BLOCK
    ri_o[...] = rows_of(
        [place, coh_row.astype(F32), base_lapse, local.astype(F32), prod_row.astype(F32)], points
    )

    step = 128
    for i in range(blocks):
        for c in copies_in(i):
            c.wait()
        for j in range(size // step):
            at = pl.ds(i * size + j * step, step)
            left = lm[at, :]
            f, b = fb[at, :], bb[at, :]
            for t in range(0, months, 2):
                growth = matmul(left, rm[:, t * 128 : (t + 2) * 128])
                f = f * growth[:, :128]
                b = jnp.maximum(b, f)
                f = f * growth[:, 128:]
                b = jnp.maximum(b, f)
            scale = matmul(left, rm[:, months * 128 : (months + 1) * 128])
            f, b = f * scale, b * scale
            s = 1.0 - lb[at, :] / 12.0
            s2 = s * s
            s4 = s2 * s2
            n = ib[at, :] * (s4 * s4 * s4)
            fb[at, :], bb[at, :], ib[at, :] = f, b, n
            w_hi, w_lo = split2(n * f)
            wsb[at, 0:128], wsb[at, 128:256] = w_hi.astype(BF16), w_lo.astype(BF16)
            s_hi, s_lo = split2(n * b)
            ssb[at, 0:128], ssb[at, 128:256] = s_hi.astype(BF16), s_lo.astype(BF16)
        for c in copies_out(i):
            c.start()
    for i in range(blocks):
        for c in copies_out(i):
            c.wait()


def value_kernel(
    ws_h, ss_h, ri, sh, sigma, vol, mix,
    lapse_o, cost_o,
    wsv, ssv, hot, sb, rb, wmat, mh, ml, zs, zr, own,
    p1s, p1r, p2s, p2r, lhs, lfv, cb, pick, brow, out,
    sem_in, sem_out, x_s, x_r, z_s, z_r, a_s, a_r, y_s, y_r, c_s, c_r, o_s, o_r, f_s, f_r,
):
    points = ri.shape[1]
    me, col = lax.axis_index("proj"), lax.axis_index("scen")
    h, u = lax.div(me, PLANE), lax.rem(me, PLANE)
    y, zl = lax.div(col, RUN_Z), lax.rem(col, RUN_Z)
    across = (1 - h) * PLANE + u
    peers = [h * PLANE + lax.rem(u + r, PLANE) for r in range(1, PLANE)]
    z_peers = [y * RUN_Z + lax.rem(zl + r, RUN_Z) for r in range(1, RUN_Z)]
    y_peers = [lax.rem(y + r, RING_Y) * RUN_Z + zl for r in range(1, RING_Y)]

    barrier = pltpu.get_barrier_semaphore()
    for p in [*peers, across]:
        pl.semaphore_signal(barrier, inc=1, device_id={"proj": p}, device_id_type=MESH)
    for p in [*z_peers, *y_peers]:
        pl.semaphore_signal(barrier, inc=1, device_id={"scen": p}, device_id_type=MESH)

    ins = [
        pltpu.make_async_copy(ws_h, wsv, sem_in.at[0]),
        pltpu.make_async_copy(ss_h, ssv, sem_in.at[1]),
    ]
    for c in ins:
        c.start()

    lane = lax.broadcasted_iota(jnp.int32, (8, 128), 1)
    place, coh_row = ri[0:1, :], ri[1:2, :]
    row16 = lax.broadcasted_iota(jnp.int32, (16, points), 0)

    first = sh[:, 0, :]
    paths = jnp.concatenate([first, first + sh[:, 1, :]], axis=0)
    spread = jnp.concatenate([paths] * RUN_Z, axis=1)
    lane16 = lax.broadcasted_iota(jnp.int32, (16, 128), 1)
    p1s[...] = jnp.where(lax.div(lane16, 128 // RUN_Z) == zl, spread, 0.0)

    m = mix[...]
    mix_norm = m / jnp.sum(m, axis=0, keepdims=True)
    mix_pair = jnp.concatenate(split2(mix_norm), axis=0).astype(BF16)
    labels = rows_of([ri[3:4, :], ri[4:5, :]], points).astype(BF16)

    def to_proj(src, dst, s, r, p):
        return pltpu.make_async_remote_copy(
            src_ref=src, dst_ref=dst, send_sem=s, recv_sem=r,
            device_id={"proj": p}, device_id_type=MESH,
        )

    def to_scen(src, dst, s, r, p):
        return pltpu.make_async_remote_copy(
            src_ref=src, dst_ref=dst, send_sem=s, recv_sem=r,
            device_id={"scen": p}, device_id_type=MESH,
        )

    def one_hots(plane):
        def values(i, _):
            want = (row16 + (plane * (PLANE * SHARE) + i * 16)).astype(F32)
            hot[pl.ds(pl.multiple_of(i * 16, 16), 16), :] = jnp.where(
                place == want, 1.0, 0.0
            ).astype(BF16)
            return 0

        def sums(i, _):
            want = (row16 + (plane * (PLANE * BLOCK) + i * 16)).astype(F32)
            hot[pl.ds(pl.multiple_of(PLANE * SHARE + i * 16, 16), 16), :] = jnp.where(
                coh_row == want, 1.0, 0.0
            ).astype(BF16)
            return 0

        lax.fori_loop(0, PLANE * SHARE // 16, values, 0)
        lax.fori_loop(0, PLANE * BLOCK // 16, sums, 0)

    def pack(k):
        got = matmul(hot[0 : PLANE * SHARE, :], wsv[...])
        for b in range(PLANE):
            part = got[b * SHARE : (b + 1) * SHARE]
            sb[k, b, 0:SHARE, :] = part[:, :128] + part[:, 128:]
        got = matmul(hot[PLANE * SHARE :, :], ssv[...])
        for b in range(PLANE):
            part = got[b * BLOCK : (b + 1) * BLOCK]
            sb[k, b, SHARE : SHARE + BLOCK, :] = part[:, :128] + part[:, 128:]
        lab = lax.dot_general(
            labels, hot[0 : PLANE * SHARE, :], (((1,), (1,)), ((), ())),
            preferred_element_type=F32,
        )
        for i in range(PLANE // 2):
            x = lab[:, i * 128 : (i + 1) * 128]
            back = pltpu.roll(x, 64, 1)
            sb[k, 2 * i, SHARE + BLOCK :, :] = jnp.where(lane < 64, x, back)
            sb[k, 2 * i + 1, SHARE + BLOCK :, :] = jnp.where(lane < 64, back, x)

    def send(k):
        sent = []
        for r in range(1, PLANE):
            sent.append(
                to_proj(
                    sb.at[k, lax.rem(u + r, PLANE)], rb.at[k, r - 1],
                    x_s.at[k, r - 1], x_r.at[k, r - 1], peers[r - 1],
                )
            )
            sent[-1].start()
        return sent

    def partial(k, dst):
        labs = []
        total = sb[k, u, SHARE : SHARE + BLOCK, :]
        for n in range(PLANE):
            mine = n == PLANE - 1
            part = sb[k, u, 0:SHARE, :] if mine else rb[k, n, 0:SHARE, :]
            hi, lo = split2(part)
            wmat[n * SHARE : (n + 1) * SHARE, 0:128] = hi.astype(BF16)
            wmat[n * SHARE : (n + 1) * SHARE, 128:256] = lo.astype(BF16)
            labs.append(sb[k, u, SHARE + BLOCK :, :] if mine else rb[k, n, SHARE + BLOCK :, :])
            if not mine:
                total = total + rb[k, n, SHARE : SHARE + BLOCK, :]
        lab = jnp.concatenate(
            [jnp.where(lane < 64, labs[2 * i], labs[2 * i + 1]) for i in range(PLANE // 2)], axis=1
        )
        arrived = PLANE * SHARE
        here, which = lab[0:1, :], lab[1:2, :]
        prod_hot = jnp.where(
            lax.broadcasted_iota(jnp.int32, (mix.shape[1], arrived), 0).astype(F32) == which,
            1.0, 0.0,
        ).astype(BF16)
        pair = matmul(mix_pair, prod_hot)
        m_hi, m_lo = pair[0:8], pair[8:16]

        def members(i, _):
            even = here == (2 * i).astype(F32)
            odd = here == (2 * i + 1).astype(F32)
            at = pl.ds(pl.multiple_of(i * 16, 16), 16)
            for ref, v in ((mh, m_hi), (ml, m_lo)):
                ref[at, :] = jnp.concatenate(
                    [jnp.where(even, v, 0.0), jnp.where(odd, v, 0.0)], axis=0
                ).astype(BF16)
            return 0

        lax.fori_loop(0, BLOCK // 2, members, 0)
        both = matmul(mh[...], wmat[...])
        sums = both[:, :128] + both[:, 128:] + matmul(ml[...], wmat[:, 0:128])
        for j in range(CHUNKS):
            dst[j, 0 : CHUNK * 8, :] = sums[j * CHUNK * 8 : (j + 1) * CHUNK * 8]
            dst[j, CHUNK * 8 :, :] = total[j * CHUNK : (j + 1) * CHUNK]

    one_hots(1 - h)
    for c in ins:
        c.wait()
    pack(0)
    pl.semaphore_wait(barrier, len(peers) + 1 + len(z_peers) + len(y_peers))
    x_sent = [send(0)]
    a_sent = [
        to_scen(p1s, p1r.at[r], a_s.at[r], a_r.at[r], z_peers[r]) for r in range(RUN_Z - 1)
    ]
    for c in a_sent:
        c.start()
    one_hots(h)
    pack(1)
    x_sent.append(send(1))

    for c in a_sent:
        c.wait_recv()
    p2s[...] = p1s[...] + p1r[0] + p1r[1] + p1r[2]
    y_sent = [
        to_scen(p2s, p2r.at[r], y_s.at[r], y_r.at[r], y_peers[r]) for r in range(RING_Y - 1)
    ]
    for c in y_sent:
        c.start()

    cols = ri[...].T
    brow[...] = jnp.broadcast_to(cols[:, 2:3], brow.shape)
    coh_col = cols[:, 1:2]
    for n in range(pick.shape[1] // 128):
        cohorts = (lax.broadcasted_iota(jnp.int32, (points, 128), 1) + n * 128).astype(F32)
        pick[:, n * 128 : (n + 1) * 128] = jnp.where(coh_col == cohorts, 1.0, 0.0).astype(BF16)

    for c in x_sent[0]:
        c.wait_recv()
    partial(0, zs)
    z_sent = [
        to_proj(zs.at[j], zr.at[j], z_s.at[j], z_r.at[j], across) for j in range(CHUNKS)
    ]
    for c in z_sent:
        c.start()

    for c in y_sent:
        c.wait_recv()
    row8 = lax.broadcasted_iota(jnp.int32, (8, 128), 0)
    for n in range(RING_Y):
        tile = p2s[...] if n == RING_Y - 1 else p2r[n]
        for k in range(2):
            hi, lo = split2(tile[k * 8 : (k + 1) * 8])
            years = jnp.where(row8 < 3, float(k + 1), 0.0)
            full = jnp.concatenate([hi, hi, lo, years], axis=0)
            at = (k * RING_Y + n) * 128
            lhs[at : at + 128, :] = full.T.astype(BF16)

    for c in x_sent[1]:
        c.wait_recv()
    partial(1, own)

    trials = RING_Y * 128
    vols = rows_of([vol[f] for f in range(8)], 128)
    sig = sigma[...]
    level = sig * LOG2E
    drift = sig * sig * (-0.5 * LOG2E)
    c_sent = []
    for j in range(CHUNKS):
        z_sent[j].wait_recv()

        def price(i, _):
            tiles, money = [], []
            for e in range(2):
                c = i * 2 + e
                at = pl.ds(pl.multiple_of(c * 8, 8), 8)
                s = own[j, at, :] + zr[j, at, :]
                g = own[j, pl.ds(CHUNK * 8 + c, 1), :] + zr[j, pl.ds(CHUNK * 8 + c, 1), :]
                inv = 1.0 / jnp.sum(s, axis=0, keepdims=True)
                loads = s * inv * vols
                d = drift * jnp.sum(loads * loads, axis=0, keepdims=True)
                a_hi, a_lo = split2(loads * level)
                tiles.append(
                    jnp.concatenate([a_hi, a_lo, a_hi, rows_of(split3(d), 128)], axis=0)
                )
                money.append(g * inv)
            right = jnp.concatenate(tiles, axis=1).astype(BF16)
            strike = jnp.concatenate(money, axis=1)
            cost = jnp.zeros((1, 256), F32)
            for k in range(2):
                acc = jnp.zeros((8, 256), F32)
                for b in range(0, trials, 256):
                    at = k * trials + b
                    x = matmul(lhs[at : at + 256, :], right)
                    pay = jnp.maximum(strike - jnp.exp2(x), 0.0)
                    acc = acc + jnp.sum(pay.reshape(32, 8, 256), axis=0)
                cost = cost + jnp.sum(acc, axis=0, keepdims=True) * (0.96 ** (k + 1) / trials)
            factor = 0.3 + 2.0 / (1.0 + jnp.exp(5.0 * cost - 2.0))
            for e in range(2):
                at = pl.ds(j * CHUNK + i * 2 + e, 1)
                cost_o[at, :] = cost[:, e * 128 : (e + 1) * 128]
                lfv[at, :] = factor[:, e * 128 : (e + 1) * 128]
            return 0

        lax.fori_loop(0, CHUNK // 2, price, 0)
        c_sent.append(
            to_proj(
                lfv.at[pl.ds(j * CHUNK, CHUNK)],
                cb.at[pl.ds(pl.multiple_of(me * BLOCK + j * CHUNK, 8), CHUNK)],
                c_s.at[j], c_r.at[j], across,
            )
        )
        c_sent[-1].start()

    o_sent = [
        to_proj(
            lfv, cb.at[pl.ds(pl.multiple_of(me * BLOCK, 8), BLOCK)],
            o_s.at[r], o_r.at[r], peers[r],
        )
        for r in range(PLANE - 1)
    ]
    for c in o_sent:
        c.start()
    cb[pl.ds(pl.multiple_of(me * BLOCK, 8), BLOCK), :] = lfv[...]
    f_sent = []
    half = BLOCK // 2
    for n in range(2):
        for j in range(n * CHUNKS // 2, (n + 1) * CHUNKS // 2):
            c_sent[j].wait_recv()
        at = pl.ds(pl.multiple_of(across * BLOCK + n * half, 8), half)
        for r in range(PLANE - 1):
            f_sent.append(to_proj(cb.at[at], cb.at[at], f_s.at[n, r], f_r.at[n, r], peers[r]))
            f_sent[-1].start()
    for c in [*o_sent, *f_sent]:
        c.wait_recv()

    hi, lo = split2(cb[...])
    factors = jnp.concatenate([hi, lo], axis=1).astype(BF16)
    blocks = sem_out.shape[0]
    size = points // blocks
    outs = []
    for i in range(blocks):
        at = pl.ds(i * size, size)
        got = matmul(pick[at, :], factors)
        out[at, :] = (got[:, :128] + got[:, 128:]) * brow[at, :]
        outs.append(pltpu.make_async_copy(out.at[at], lapse_o.at[at], sem_out.at[i]))
        outs[-1].start()
    for c in [*x_sent[0], *x_sent[1], *a_sent, *y_sent, *z_sent, *c_sent, *o_sent, *f_sent]:
        c.wait_send()
    for c in outs:
        c.wait()


def body(
    fund_value, in_force, guarantee_base, lapse_rate, cohort, product, guarantee_type,
    returns, mix_table, fee_table, rollup_table, fund_vol, closing_sigma_figure, shocks,
    base_table, year_index,
):
    points, scens = fund_value.shape
    cohorts = BLOCK * lax.axis_size("proj")
    blocks = 4
    vmem = pl.BlockSpec(memory_space=pltpu.VMEM)
    smem = pl.BlockSpec(memory_space=pltpu.SMEM)
    hbm = pl.BlockSpec(memory_space=pl.ANY)
    dma = pltpu.SemaphoreType.DMA
    full = jax.ShapeDtypeStruct((points, scens), F32)
    pair = jax.ShapeDtypeStruct((points, 2 * scens), BF16)
    months = returns.shape[1]
    fund_next, force_next, base_next, ws, ss, ri = pl.pallas_call(
        functools.partial(project_kernel, blocks),
        out_shape=(full, full, full, pair, pair, jax.ShapeDtypeStruct((8, points), F32)),
        in_specs=[hbm] * 4 + [vmem] * 5 + [smem] * 2 + [vmem, smem],
        out_specs=(hbm,) * 5 + (vmem,),
        scratch_shapes=[
            *[pltpu.VMEM((points, scens), F32)] * 4,
            *[pltpu.VMEM((points, 2 * scens), BF16)] * 2,
            pltpu.VMEM((points, KDIM), BF16),
            pltpu.VMEM((KDIM, (months + 1) * scens), BF16),
            dma((blocks, 4)),
            dma((blocks, 5)),
        ],
    )(
        fund_value, in_force, guarantee_base, lapse_rate,
        cohort.reshape(1, points), product.reshape(1, points), guarantee_type.reshape(1, points),
        returns.transpose(1, 0, 2), mix_table.T, fee_table, rollup_table, base_table, year_index,
    )
    lapse_next, cost = pl.pallas_call(
        value_kernel,
        out_shape=(full, jax.ShapeDtypeStruct((BLOCK, scens), F32)),
        in_specs=[hbm] * 2 + [vmem] * 3 + [smem, vmem],
        out_specs=(hbm, vmem),
        scratch_shapes=[
            *[pltpu.VMEM((points, 2 * scens), BF16)] * 2,
            pltpu.VMEM((PLANE * (SHARE + BLOCK), points), BF16),
            pltpu.VMEM((2, PLANE, ROWS, scens), F32),
            pltpu.VMEM((2, PLANE - 1, ROWS, scens), F32),
            pltpu.VMEM((PLANE * SHARE, 2 * scens), BF16),
            *[pltpu.VMEM((BLOCK * 8, PLANE * SHARE), BF16)] * 2,
            *[pltpu.VMEM((CHUNKS, PART, scens), F32)] * 3,
            pltpu.VMEM((16, 128), F32),
            pltpu.VMEM((RUN_Z - 1, 16, 128), F32),
            pltpu.VMEM((16, 128), F32),
            pltpu.VMEM((RING_Y - 1, 16, 128), F32),
            pltpu.VMEM((2 * RING_Y * 128, KDIM), BF16),
            pltpu.VMEM((BLOCK, scens), F32),
            pltpu.VMEM((cohorts, scens), F32),
            pltpu.VMEM((points, cohorts), BF16),
            pltpu.VMEM((points, scens), F32),
            pltpu.VMEM((points, scens), F32),
            dma((2,)),
            dma((4,)),
            *[dma((2, PLANE - 1))] * 2,
            *[dma((CHUNKS,))] * 2,
            *[dma((RUN_Z - 1,))] * 2,
            *[dma((RING_Y - 1,))] * 2,
            *[dma((CHUNKS,))] * 2,
            *[dma((PLANE - 1,))] * 2,
            *[dma((2, PLANE - 1))] * 2,
        ],
        compiler_params=pltpu.CompilerParams(collective_id=0, has_side_effects=True),
    )(ws, ss, ri, shocks, closing_sigma_figure.reshape(1, scens), fund_vol, mix_table.T)
    return fund_next, force_next, base_next, lapse_next, cost


def solution(mesh):
    wide, row, last = P("proj", "scen"), P("proj"), P(None, None, "scen")
    placed = (
        wide, wide, wide, wide, row, row, row, last,
        P(), P(), P(), P(), P("scen"), last, P(), P(),
    )
    return jax.shard_map(
        body, mesh=mesh, in_specs=placed, out_specs=(wide,) * 5, check_vma=False
    )
```

```python
import functools

import jax
import jax.numpy as jnp
from jax import lax
from jax.experimental import pallas as pl
from jax.experimental.pallas import tpu as pltpu
from jax.sharding import PartitionSpec as P

F32, BF16 = jnp.float32, jnp.bfloat16
MESH = pl.DeviceIdType.MESH
LOG2E = 1.4426950408889634

PLANES, PLANE = 2, 8
RING_Y, RUN_Z = 8, 4
SHARE, BLOCK = 64, 32
ROWS = SHARE + BLOCK
CHUNKS, CHUNK = 4, 8
PART = CHUNK * 8 + CHUNK
KDIM = 32


def split2(x):
    hi = x.astype(BF16).astype(F32)
    return hi, x - hi


def split3(x):
    hi, rest = split2(x)
    mid, lo = split2(rest)
    return hi, mid, lo


def matmul(a, b):
    return jnp.dot(a, b, preferred_element_type=F32)


def rows_of(pieces, lanes):
    row = lax.broadcasted_iota(jnp.int32, (8, lanes), 0)
    out = jnp.zeros((8, lanes), F32)
    for i, piece in enumerate(pieces):
        out = jnp.where(row == i, piece, out)
    return out


def main_kernel(
    blocks,
    fund, force, base, lapse, coh_h, prod_h, gtype_h, ret_h, mix_h, table_h, sh_h, sigma_h,
    fee_h, roll_h, vol_h, year,
    fund_o, force_o, base_o, pick, brow, cb, cost_o,
    lb, coh, prod, gtype, ret, mix, table, sh, sigma, fee, roll, vol,
    lm, rm, wsv, ssv, hot, sl, rl, sb, rb, wmat, mh, ml, zs, zr, own,
    p1s, p1r, p2s, p2r, lhs, lfv,
    sem_small, sem_in,
    l_s, l_r, x_s, x_r, z_s, z_r, a_s, a_r, y_s, y_r, c_s, c_r,
):
    points = lb.shape[0]
    size = points // blocks
    months = ret.shape[0]
    me, col = lax.axis_index("proj"), lax.axis_index("scen")
    h, u = lax.div(me, PLANE), lax.rem(me, PLANE)
    y, zl = lax.div(col, RUN_Z), lax.rem(col, RUN_Z)
    across = (1 - h) * PLANE + u
    peers = [h * PLANE + lax.rem(u + r, PLANE) for r in range(1, PLANE)]
    far = [(1 - h) * PLANE + lax.rem(u + r, PLANE) for r in range(1, PLANE)]
    z_peers = [y * RUN_Z + lax.rem(zl + r, RUN_Z) for r in range(1, RUN_Z)]
    y_peers = [lax.rem(y + r, RING_Y) * RUN_Z + zl for r in range(1, RING_Y)]

    barrier = pltpu.get_barrier_semaphore()
    for p in [*far, across, *peers]:
        pl.semaphore_signal(barrier, inc=1, device_id={"proj": p}, device_id_type=MESH)
    for p in [*z_peers, *y_peers]:
        pl.semaphore_signal(barrier, inc=1, device_id={"scen": p}, device_id_type=MESH)

    smalls = [
        pltpu.make_async_copy(src, dst, sem_small.at[n])
        for n, (src, dst) in enumerate((
            (coh_h, coh), (prod_h, prod), (gtype_h, gtype), (mix_h, mix), (fee_h, fee),
            (roll_h, roll), (vol_h, vol), (ret_h, ret), (table_h, table),
            (sh_h, sh), (sigma_h, sigma),
        ))
    ]

    def copies_in(i):
        at = pl.ds(i * size, size)
        return [
            pltpu.make_async_copy(src.at[at], dst.at[at], sem_in.at[i, n])
            for n, (src, dst) in enumerate(
                ((fund, fund_o), (base, base_o), (force, force_o), (lapse, lb))
            )
        ]

    for c in smalls:
        c.start()
    for i in range(blocks):
        for c in copies_in(i):
            c.start()
    for c in smalls:
        c.wait()

    lane = lax.broadcasted_iota(jnp.int32, (8, 128), 1)
    row8 = lax.broadcasted_iota(jnp.int32, (8, 128), 0)
    row16 = lax.broadcasted_iota(jnp.int32, (16, points), 0)

    owners = points // SHARE
    coh_row = coh[...]
    owner_row = lax.div(coh_row, BLOCK)
    owner_iota = lax.broadcasted_iota(jnp.int32, (owners, points), 0)
    owner_hot = jnp.where(owner_iota == owner_row, 1.0, 0.0)
    before = jnp.where(
        lax.broadcasted_iota(jnp.int32, (128, 128), 0)
        < lax.broadcasted_iota(jnp.int32, (128, 128), 1),
        1.0, 0.0,
    ).astype(BF16)
    offset = lax.broadcasted_iota(jnp.int32, (owners, 1), 0).astype(F32) * float(SHARE)
    places = []
    for b in range(points // 128):
        part = owner_hot[:, b * 128 : (b + 1) * 128]
        rank = matmul(part.astype(BF16), before) + offset
        places.append(jnp.sum(part * rank, axis=0, keepdims=True))
        offset = offset + jnp.sum(part, axis=1, keepdims=True)
    place = jnp.concatenate(places, axis=1)
    prod_row = prod[...]
    coh_f = coh_row.astype(F32)
    labels = rows_of(
        [(coh_row - owner_row * BLOCK).astype(F32), prod_row.astype(F32)], points
    ).astype(BF16)

    for k in range(2):
        plane = 1 - h if k == 0 else h

        def values(i, _):
            want = (row16 + (plane * (PLANE * SHARE) + i * 16)).astype(F32)
            hot[k, pl.ds(pl.multiple_of(i * 16, 16), 16), :] = jnp.where(
                place == want, 1.0, 0.0
            ).astype(BF16)
            return 0

        def sums(i, _):
            want = (row16 + (plane * (PLANE * BLOCK) + i * 16)).astype(F32)
            hot[k, pl.ds(pl.multiple_of(PLANE * SHARE + i * 16, 16), 16), :] = jnp.where(
                coh_f == want, 1.0, 0.0
            ).astype(BF16)
            return 0

        lax.fori_loop(0, PLANE * SHARE // 16, values, 0)
        lax.fori_loop(0, PLANE * BLOCK // 16, sums, 0)
        lab = lax.dot_general(
            labels, hot[k, 0 : PLANE * SHARE, :], (((1,), (1,)), ((), ())),
            preferred_element_type=F32,
        )
        for i in range(PLANE // 2):
            x = lab[:, i * 128 : (i + 1) * 128]
            back = pltpu.roll(x, 64, 1)
            sl[k, 2 * i] = jnp.where(lane < 64, x, back)
            sl[k, 2 * i + 1] = jnp.where(lane < 64, back, x)

    products = mix.shape[1]
    m = mix[...]
    mix_norm = m / jnp.sum(m, axis=0, keepdims=True)
    prod_hot = jnp.where(
        lax.broadcasted_iota(jnp.int32, (products, points), 0) == prod_row, 1.0, 0.0
    )
    mix_rows = jnp.dot(
        mix_norm, prod_hot, precision=lax.Precision.HIGHEST, preferred_element_type=F32
    )
    g = gtype[...]
    fee_row, roll_row = jnp.zeros(g.shape, F32), jnp.zeros(g.shape, F32)
    for k in range(fee.shape[0]):
        fee_row = jnp.where(g == k, fee[k], fee_row)
        roll_row = jnp.where(g == k, roll[k], roll_row)
    grow = 1.0 + roll_row / 12.0
    kappa = (1.0 - fee_row) / grow
    g2 = grow * grow
    g4 = g2 * g2
    grow_year = g4 * g4 * g4
    a_hi, a_lo = split2(mix_rows * kappa)
    extra = rows_of([*split3(kappa), *split3(grow_year)], points)
    left_rows = jnp.concatenate([a_hi, a_hi, a_lo, extra], axis=0)
    lm[...] = left_rows.T.astype(BF16)
    ones = jnp.where(row8 < 3, 1.0, 0.0)
    for t in range(months):
        r_hi, r_lo = split2(ret[t])
        tile = jnp.concatenate([r_hi, r_lo, r_hi, ones], axis=0)
        rm[:, t * 128 : (t + 1) * 128] = tile.astype(BF16)
    last = jnp.where((row8 >= 3) & (row8 < 6), 1.0, 0.0)
    zero = jnp.zeros((8, 128), F32)
    rm[:, months * 128 : (months + 1) * 128] = jnp.concatenate(
        [zero, zero, zero, last], axis=0
    ).astype(BF16)

    first = sh[:, 0, :]
    paths = jnp.concatenate([first, first + sh[:, 1, :]], axis=0)
    spread = jnp.concatenate([paths] * RUN_Z, axis=1)
    lane16 = lax.broadcasted_iota(jnp.int32, (16, 128), 1)
    p1s[...] = jnp.where(lax.div(lane16, 128 // RUN_Z) == zl, spread, 0.0)

    def to_proj(src, dst, s, r, p):
        return pltpu.make_async_remote_copy(
            src_ref=src, dst_ref=dst, send_sem=s, recv_sem=r,
            device_id={"proj": p}, device_id_type=MESH,
        )

    def to_scen(src, dst, s, r, p):
        return pltpu.make_async_remote_copy(
            src_ref=src, dst_ref=dst, send_sem=s, recv_sem=r,
            device_id={"scen": p}, device_id_type=MESH,
        )

    pl.semaphore_wait(barrier, 2 * PLANE - 1 + len(z_peers) + len(y_peers))
    l_sent = [[], []]
    for k in range(2):
        for r in range(1, PLANE):
            l_sent[k].append(
                to_proj(
                    sl.at[k, lax.rem(u + r, PLANE)], rl.at[k, r - 1],
                    l_s.at[k, r - 1], l_r.at[k, r - 1], peers[r - 1],
                )
            )
            l_sent[k][-1].start()
    a_sent = [
        to_scen(p1s, p1r.at[r], a_s.at[r], a_r.at[r], z_peers[r]) for r in range(RUN_Z - 1)
    ]
    for c in a_sent:
        c.start()

    step = 128
    for i in range(blocks):
        for c in copies_in(i):
            c.wait()
        for j in range(size // step):
            at = pl.ds(i * size + j * step, step)
            left = lm[at, :]
            f, b = fund_o[at, :], base_o[at, :]
            for t in range(0, months, 2):
                growth = matmul(left, rm[:, t * 128 : (t + 2) * 128])
                f = f * growth[:, :128]
                b = jnp.maximum(b, f)
                f = f * growth[:, 128:]
                b = jnp.maximum(b, f)
            scale = matmul(left, rm[:, months * 128 : (months + 1) * 128])
            f, b = f * scale, b * scale
            s = 1.0 - lb[at, :] / 12.0
            s2 = s * s
            s4 = s2 * s2
            n = force_o[at, :] * (s4 * s4 * s4)
            fund_o[at, :], base_o[at, :], force_o[at, :] = f, b, n
            w_hi, w_lo = split2(n * f)
            wsv[at, 0:128], wsv[at, 128:256] = w_hi.astype(BF16), w_lo.astype(BF16)
            s_hi, s_lo = split2(n * b)
            ssv[at, 0:128], ssv[at, 128:256] = s_hi.astype(BF16), s_lo.astype(BF16)

    x_sent = [[], []]
    for k in range(2):
        got = matmul(hot[k, 0 : PLANE * SHARE, :], wsv[...])
        for b in range(PLANE):
            part = got[b * SHARE : (b + 1) * SHARE]
            sb[k, b, 0:SHARE, :] = part[:, :128] + part[:, 128:]
        got = matmul(hot[k, PLANE * SHARE :, :], ssv[...])
        for b in range(PLANE):
            part = got[b * BLOCK : (b + 1) * BLOCK]
            sb[k, b, SHARE:, :] = part[:, :128] + part[:, 128:]
        for r in range(1, PLANE):
            x_sent[k].append(
                to_proj(
                    sb.at[k, lax.rem(u + r, PLANE)], rb.at[k, r - 1],
                    x_s.at[k, r - 1], x_r.at[k, r - 1], peers[r - 1],
                )
            )
            x_sent[k][-1].start()

    for c in a_sent:
        c.wait_recv()
    p2s[...] = p1s[...] + p1r[0] + p1r[1] + p1r[2]
    y_sent = [
        to_scen(p2s, p2r.at[r], y_s.at[r], y_r.at[r], y_peers[r]) for r in range(RING_Y - 1)
    ]
    for c in y_sent:
        c.start()

    mix_pair = jnp.concatenate(split2(mix_norm), axis=0).astype(BF16)
    for k in range(2):
        for c in l_sent[k]:
            c.wait_recv()
        labs = [rl[k, n] for n in range(PLANE - 1)] + [sl[k, u]]
        lab = jnp.concatenate(
            [jnp.where(lane < 64, labs[2 * i], labs[2 * i + 1]) for i in range(PLANE // 2)], axis=1
        )
        here, which = lab[0:1, :], lab[1:2, :]
        arrived_hot = jnp.where(
            lax.broadcasted_iota(jnp.int32, (products, PLANE * SHARE), 0).astype(F32) == which,
            1.0, 0.0,
        ).astype(BF16)
        pair = matmul(mix_pair, arrived_hot)
        m_hi, m_lo = pair[0:8], pair[8:16]

        def members(i, _):
            even = here == (2 * i).astype(F32)
            odd = here == (2 * i + 1).astype(F32)
            at = pl.ds(pl.multiple_of(i * 16, 16), 16)
            for ref, v in ((mh, m_hi), (ml, m_lo)):
                ref[k, at, :] = jnp.concatenate(
                    [jnp.where(even, v, 0.0), jnp.where(odd, v, 0.0)], axis=0
                ).astype(BF16)
            return 0

        lax.fori_loop(0, BLOCK // 2, members, 0)

    def partial(k, dst):
        for c in x_sent[k]:
            c.wait_recv()
        total = sb[k, u, SHARE:, :]
        for n in range(PLANE):
            mine = n == PLANE - 1
            hi, lo = split2(sb[k, u, 0:SHARE, :] if mine else rb[k, n, 0:SHARE, :])
            wmat[n * SHARE : (n + 1) * SHARE, 0:128] = hi.astype(BF16)
            wmat[n * SHARE : (n + 1) * SHARE, 128:256] = lo.astype(BF16)
            if not mine:
                total = total + rb[k, n, SHARE:, :]
        both = matmul(mh[k], wmat[...])
        sums = both[:, :128] + both[:, 128:] + matmul(ml[k], wmat[:, 0:128])
        for j in range(CHUNKS):
            dst[j, 0 : CHUNK * 8, :] = sums[j * CHUNK * 8 : (j + 1) * CHUNK * 8]
            dst[j, CHUNK * 8 :, :] = total[j * CHUNK : (j + 1) * CHUNK]

    partial(0, zs)
    z_sent = [
        to_proj(zs.at[j], zr.at[j], z_s.at[j], z_r.at[j], across) for j in range(CHUNKS)
    ]
    for c in z_sent:
        c.start()

    lapses = jnp.dot(
        table[...], prod_hot, precision=lax.Precision.HIGHEST, preferred_element_type=F32
    )
    picked = lax.broadcasted_iota(jnp.int32, lapses.shape, 0) == year[0]
    base_lapse = jnp.sum(jnp.where(picked, lapses, 0.0), axis=0, keepdims=True)
    cols = rows_of([coh_f, base_lapse], points).T
    brow[...] = jnp.broadcast_to(cols[:, 1:2], brow.shape)
    coh_col = cols[:, 0:1]
    for n in range(pick.shape[1] // 128):
        cohorts = (lax.broadcasted_iota(jnp.int32, (points, 128), 1) + n * 128).astype(F32)
        pick[:, n * 128 : (n + 1) * 128] = jnp.where(coh_col == cohorts, 1.0, 0.0).astype(BF16)

    for c in y_sent:
        c.wait_recv()
    for n in range(RING_Y):
        tile = p2s[...] if n == RING_Y - 1 else p2r[n]
        for k in range(2):
            hi, lo = split2(tile[k * 8 : (k + 1) * 8])
            years = jnp.where(row8 < 3, float(k + 1), 0.0)
            full = jnp.concatenate([hi, hi, lo, years], axis=0)
            at = (k * RING_Y + n) * 128
            lhs[at : at + 128, :] = full.T.astype(BF16)

    partial(1, own)

    trials = RING_Y * 128
    vols = rows_of([vol[f] for f in range(8)], 128)
    sig = sigma[...]
    level = sig * LOG2E
    drift = sig * sig * (-0.5 * LOG2E)
    c_sent = []
    for j in range(CHUNKS):
        z_sent[j].wait_recv()

        def price(i, _):
            tiles, money = [], []
            for e in range(2):
                c = i * 2 + e
                at = pl.ds(pl.multiple_of(c * 8, 8), 8)
                s = own[j, at, :] + zr[j, at, :]
                g = own[j, pl.ds(CHUNK * 8 + c, 1), :] + zr[j, pl.ds(CHUNK * 8 + c, 1), :]
                inv = 1.0 / jnp.sum(s, axis=0, keepdims=True)
                loads = s * inv * vols
                d = drift * jnp.sum(loads * loads, axis=0, keepdims=True)
                a_hi, a_lo = split2(loads * level)
                tiles.append(
                    jnp.concatenate([a_hi, a_lo, a_hi, rows_of(split3(d), 128)], axis=0)
                )
                money.append(g * inv)
            right = jnp.concatenate(tiles, axis=1).astype(BF16)
            strike = jnp.concatenate(money, axis=1)
            cost = jnp.zeros((1, 256), F32)
            for k in range(2):
                acc = jnp.zeros((8, 256), F32)
                for b in range(0, trials, 256):
                    at = k * trials + b
                    x = matmul(lhs[at : at + 256, :], right)
                    pay = jnp.maximum(strike - jnp.exp2(x), 0.0)
                    acc = acc + jnp.sum(pay.reshape(32, 8, 256), axis=0)
                cost = cost + jnp.sum(acc, axis=0, keepdims=True) * (0.96 ** (k + 1) / trials)
            factor = 0.3 + 2.0 / (1.0 + jnp.exp(5.0 * cost - 2.0))
            for e in range(2):
                at = pl.ds(j * CHUNK + i * 2 + e, 1)
                cost_o[at, :] = cost[:, e * 128 : (e + 1) * 128]
                lfv[at, :] = factor[:, e * 128 : (e + 1) * 128]
            return 0

        lax.fori_loop(0, CHUNK // 2, price, 0)
        for n, p in enumerate([*far, across, *peers]):
            c_sent.append(
                to_proj(
                    lfv.at[pl.ds(j * CHUNK, CHUNK)],
                    cb.at[pl.ds(pl.multiple_of(me * BLOCK + j * CHUNK, 8), CHUNK)],
                    c_s.at[j, n], c_r.at[j, n], p,
                )
            )
            c_sent[-1].start()

    cb[pl.ds(pl.multiple_of(me * BLOCK, 8), BLOCK), :] = lfv[...]
    for c in [*l_sent[0], *l_sent[1], *x_sent[0], *x_sent[1], *a_sent, *y_sent, *z_sent]:
        c.wait_send()
    for c in c_sent:
        c.wait_send()
    for c in c_sent:
        c.wait_recv()


def last_kernel(
    fund, force, base, pick, brow, cb, cost,
    fund_o, force_o, base_o, lapse_o, cost_o,
    out, sem, sem_out,
):
    outs = [
        pltpu.make_async_copy(src, dst, sem.at[n])
        for n, (src, dst) in enumerate(
            ((fund, fund_o), (force, force_o), (base, base_o), (cost, cost_o))
        )
    ]
    for c in outs:
        c.start()
    points = out.shape[0]
    factors = jnp.concatenate(split2(cb[...]), axis=1).astype(BF16)
    blocks = sem_out.shape[0]
    size = points // blocks
    for i in range(blocks):
        at = pl.ds(i * size, size)
        got = matmul(pick[at, :], factors)
        out[at, :] = (got[:, :128] + got[:, 128:]) * brow[at, :]
        outs.append(pltpu.make_async_copy(out.at[at], lapse_o.at[at], sem_out.at[i]))
        outs[-1].start()
    for c in outs:
        c.wait()


def body(
    fund_value, in_force, guarantee_base, lapse_rate, cohort, product, guarantee_type,
    returns, mix_table, fee_table, rollup_table, fund_vol, closing_sigma_figure, shocks,
    base_table, year_index,
):
    points, scens = fund_value.shape
    cohorts = BLOCK * lax.axis_size("proj")
    blocks = 4
    vmem = pl.BlockSpec(memory_space=pltpu.VMEM)
    hbm = pl.BlockSpec(memory_space=pl.ANY)
    dma = pltpu.SemaphoreType.DMA
    full = jax.ShapeDtypeStruct((points, scens), F32)
    own = jax.ShapeDtypeStruct((BLOCK, scens), F32)
    months = returns.shape[1]
    ints = pltpu.VMEM((1, points), jnp.int32)
    args = [
        fund_value, in_force, guarantee_base, lapse_rate,
        cohort.reshape(1, points), product.reshape(1, points), guarantee_type.reshape(1, points),
        returns.transpose(1, 0, 2), mix_table.T, base_table, shocks,
        closing_sigma_figure.reshape(1, scens), fee_table, rollup_table, fund_vol,
    ]
    args = [pltpu.with_memory_space_constraint(a, pltpu.HBM) for a in args]
    middle = pl.pallas_call(
        functools.partial(main_kernel, blocks),
        out_shape=(
            full, full, full,
            jax.ShapeDtypeStruct((points, cohorts), BF16),
            full,
            jax.ShapeDtypeStruct((cohorts, scens), F32),
            own,
        ),
        in_specs=[hbm] * 15 + [pl.BlockSpec(memory_space=pltpu.SMEM)],
        out_specs=(vmem,) * 7,
        scratch_shapes=[
            pltpu.VMEM((points, scens), F32),
            ints, ints, ints,
            pltpu.VMEM((months, 8, scens), F32),
            pltpu.VMEM((8, 16), F32),
            pltpu.VMEM(base_table.shape, F32),
            pltpu.VMEM(shocks.shape, F32),
            pltpu.VMEM((1, scens), F32),
            pltpu.SMEM(fee_table.shape, F32),
            pltpu.SMEM(rollup_table.shape, F32),
            pltpu.SMEM((8,), F32),
            pltpu.VMEM((points, KDIM), BF16),
            pltpu.VMEM((KDIM, (months + 1) * scens), BF16),
            *[pltpu.VMEM((points, 2 * scens), BF16)] * 2,
            pltpu.VMEM((2, PLANE * (SHARE + BLOCK), points), BF16),
            pltpu.VMEM((2, PLANE, 8, 128), F32),
            pltpu.VMEM((2, PLANE - 1, 8, 128), F32),
            pltpu.VMEM((2, PLANE, ROWS, scens), F32),
            pltpu.VMEM((2, PLANE - 1, ROWS, scens), F32),
            pltpu.VMEM((PLANE * SHARE, 2 * scens), BF16),
            *[pltpu.VMEM((2, BLOCK * 8, PLANE * SHARE), BF16)] * 2,
            *[pltpu.VMEM((CHUNKS, PART, scens), F32)] * 3,
            pltpu.VMEM((16, 128), F32),
            pltpu.VMEM((RUN_Z - 1, 16, 128), F32),
            pltpu.VMEM((16, 128), F32),
            pltpu.VMEM((RING_Y - 1, 16, 128), F32),
            pltpu.VMEM((2 * RING_Y * 128, KDIM), BF16),
            pltpu.VMEM((BLOCK, scens), F32),
            dma((11,)),
            dma((blocks, 4)),
            *[dma((2, PLANE - 1))] * 4,
            *[dma((CHUNKS,))] * 2,
            *[dma((RUN_Z - 1,))] * 2,
            *[dma((RING_Y - 1,))] * 2,
            *[dma((CHUNKS, 2 * PLANE - 1))] * 2,
        ],
        compiler_params=pltpu.CompilerParams(
            collective_id=0, has_side_effects=True, vmem_limit_bytes=28 << 20
        ),
    )(*args, year_index)
    return pl.pallas_call(
        last_kernel,
        out_shape=(full, full, full, full, own),
        in_specs=[vmem] * 7,
        out_specs=(hbm,) * 5,
        scratch_shapes=[pltpu.VMEM((points, scens), F32), dma((4,)), dma((4,))],
        compiler_params=pltpu.CompilerParams(vmem_limit_bytes=28 << 20),
    )(*middle)


def solution(mesh):
    wide, row, last = P("proj", "scen"), P("proj"), P(None, None, "scen")
    placed = (
        wide, wide, wide, wide, row, row, row, last,
        P(), P(), P(), P(), P("scen"), last, P(), P(),
    )
    return jax.shard_map(
        body, mesh=mesh, in_specs=placed, out_specs=(wide,) * 5, check_vma=False
    )
```

```python
import functools

import jax
import jax.numpy as jnp
from jax import lax
from jax.experimental import pallas as pl
from jax.experimental.pallas import tpu as pltpu
from jax.sharding import PartitionSpec as P

F32, BF16 = jnp.float32, jnp.bfloat16
MESH = pl.DeviceIdType.MESH
LOG2E = 1.4426950408889634

PLANES, PLANE = 2, 8
RING_Y, RUN_Z = 8, 4
SHARE, BLOCK = 64, 32
ROWS = SHARE + BLOCK
CHUNKS, CHUNK = 4, 8
PART = CHUNK * 8 + CHUNK
KDIM = 32


def split2(x):
    hi = x.astype(BF16).astype(F32)
    return hi, x - hi


def split3(x):
    hi, rest = split2(x)
    mid, lo = split2(rest)
    return hi, mid, lo


def matmul(a, b):
    return jnp.dot(a, b, preferred_element_type=F32)


def rows_of(pieces, lanes):
    row = lax.broadcasted_iota(jnp.int32, (8, lanes), 0)
    out = jnp.zeros((8, lanes), F32)
    for i, piece in enumerate(pieces):
        out = jnp.where(row == i, piece, out)
    return out


def main_kernel(
    blocks,
    fund, force, base, lapse, coh_h, prod_h, gtype_h, ret_h, mix_h, table_h, sh_h, sigma_h,
    fee_h, roll_h, vol_h, year,
    fund_o, force_o, base_o, pick, brow, cb, cost_o,
    lb, coh, prod, gtype, ret, mix, table, sh, sigma, fee, roll, vol,
    lm, rm, wsv, ssv, hot, sl, rl, sb, rb, wmat, mh, ml, zs, zr, own,
    p1s, p1r, p2s, p2r, lhs, lfv,
    sem_small, sem_in,
    l_s, l_r, x_s, x_r, z_s, z_r, a_s, a_r, y_s, y_r, c_s, c_r,
):
    points = lb.shape[0]
    size = points // blocks
    months = ret.shape[0]
    me, col = lax.axis_index("proj"), lax.axis_index("scen")
    h, u = lax.div(me, PLANE), lax.rem(me, PLANE)
    y, zl = lax.div(col, RUN_Z), lax.rem(col, RUN_Z)
    across = (1 - h) * PLANE + u
    peers = [h * PLANE + lax.rem(u + r, PLANE) for r in range(1, PLANE)]
    far = [(1 - h) * PLANE + lax.rem(u + r, PLANE) for r in range(1, PLANE)]
    z_peers = [y * RUN_Z + lax.rem(zl + r, RUN_Z) for r in range(1, RUN_Z)]
    y_peers = [lax.rem(y + r, RING_Y) * RUN_Z + zl for r in range(1, RING_Y)]

    smalls = [
        pltpu.make_async_copy(src, dst, sem_small.at[n])
        for n, (src, dst) in enumerate((
            (coh_h, coh), (prod_h, prod), (gtype_h, gtype), (mix_h, mix), (fee_h, fee),
            (roll_h, roll), (vol_h, vol), (ret_h, ret), (table_h, table),
            (sh_h, sh), (sigma_h, sigma),
        ))
    ]

    def copies_in(i):
        at = pl.ds(i * size, size)
        return [
            pltpu.make_async_copy(src.at[at], dst.at[at], sem_in.at[i, n])
            for n, (src, dst) in enumerate(
                ((fund, fund_o), (base, base_o), (force, force_o), (lapse, lb))
            )
        ]

    for c in smalls:
        c.start()
    for i in range(blocks):
        for c in copies_in(i):
            c.start()

    barrier = pltpu.get_barrier_semaphore()
    for p in [*far, across, *peers]:
        pl.semaphore_signal(barrier, inc=1, device_id={"proj": p}, device_id_type=MESH)
    for p in [*z_peers, *y_peers]:
        pl.semaphore_signal(barrier, inc=1, device_id={"scen": p}, device_id_type=MESH)
    for c in smalls:
        c.wait()

    lane = lax.broadcasted_iota(jnp.int32, (8, 128), 1)
    row8 = lax.broadcasted_iota(jnp.int32, (8, 128), 0)

    owners = points // SHARE
    coh_row = coh[...]
    owner_row = lax.div(coh_row, BLOCK)
    owner_iota = lax.broadcasted_iota(jnp.int32, (owners, points), 0)
    owner_hot = jnp.where(owner_iota == owner_row, 1.0, 0.0)
    before = jnp.where(
        lax.broadcasted_iota(jnp.int32, (128, 128), 0)
        < lax.broadcasted_iota(jnp.int32, (128, 128), 1),
        1.0, 0.0,
    ).astype(BF16)
    offset = lax.broadcasted_iota(jnp.int32, (owners, 1), 0).astype(F32) * float(SHARE)
    places = []
    for b in range(points // 128):
        part = owner_hot[:, b * 128 : (b + 1) * 128]
        rank = matmul(part.astype(BF16), before) + offset
        places.append(jnp.sum(part * rank, axis=0, keepdims=True))
        offset = offset + jnp.sum(part, axis=1, keepdims=True)
    place = jnp.concatenate(places, axis=1)
    prod_row = prod[...]
    coh_f = coh_row.astype(F32)
    labels = rows_of(
        [(coh_row - owner_row * BLOCK).astype(F32), prod_row.astype(F32)], points
    ).astype(BF16)

    row16 = lax.broadcasted_iota(jnp.int32, (16, points), 0).astype(F32)
    nil = jnp.zeros((16, points), BF16)

    def tiled_hot(row):
        tile = jnp.floor(row * 0.0625)
        within = jnp.where(row16 == row - tile * 16.0, 1.0, 0.0).astype(BF16)
        return jnp.broadcast_to(tile, (16, points)).astype(BF16), within

    place_tile, place_hot = tiled_hot(place)
    coh_tile, coh_hot = tiled_hot(coh_f)

    def one_hots(k):
        plane = 1 - h if k == 0 else h

        def values(i, _):
            tile = (plane * (PLANE * SHARE // 16) + i).astype(F32).astype(BF16)
            hot[k, pl.ds(pl.multiple_of(i * 16, 16), 16), :] = jnp.where(
                place_tile == tile, place_hot, nil
            )
            return 0

        def sums(i, _):
            tile = (plane * (PLANE * BLOCK // 16) + i).astype(F32).astype(BF16)
            hot[k, pl.ds(pl.multiple_of(PLANE * SHARE + i * 16, 16), 16), :] = jnp.where(
                coh_tile == tile, coh_hot, nil
            )
            return 0

        lax.fori_loop(0, PLANE * SHARE // 16, values, 0, unroll=4)
        lax.fori_loop(0, PLANE * BLOCK // 16, sums, 0, unroll=4)
        lab = lax.dot_general(
            labels, hot[k, 0 : PLANE * SHARE, :], (((1,), (1,)), ((), ())),
            preferred_element_type=F32,
        )
        for i in range(PLANE // 2):
            x = lab[:, i * 128 : (i + 1) * 128]
            back = pltpu.roll(x, 64, 1)
            sl[k, 2 * i] = jnp.where(lane < 64, x, back)[0:2]
            sl[k, 2 * i + 1] = jnp.where(lane < 64, back, x)[0:2]

    one_hots(0)

    products = mix.shape[1]
    m = mix[...]
    mix_norm = m / jnp.sum(m, axis=0, keepdims=True)
    prod_hot = jnp.where(
        lax.broadcasted_iota(jnp.int32, (products, points), 0) == prod_row, 1.0, 0.0
    )
    mix_rows = jnp.dot(
        mix_norm, prod_hot, precision=lax.Precision.HIGHEST, preferred_element_type=F32
    )
    g = gtype[...]
    fee_row, roll_row = jnp.zeros(g.shape, F32), jnp.zeros(g.shape, F32)
    for k in range(fee.shape[0]):
        fee_row = jnp.where(g == k, fee[k], fee_row)
        roll_row = jnp.where(g == k, roll[k], roll_row)
    grow = 1.0 + roll_row / 12.0
    kappa = (1.0 - fee_row) / grow
    g2 = grow * grow
    g4 = g2 * g2
    grow_year = g4 * g4 * g4
    a_hi, a_lo = split2(mix_rows * kappa)
    extra = rows_of([*split3(kappa), *split3(grow_year)], points)
    left_rows = jnp.concatenate([a_hi, a_hi, a_lo, extra], axis=0)
    lm[...] = left_rows.T.astype(BF16)
    ones = jnp.where(row8 < 3, 1.0, 0.0)
    for t in range(months):
        r_hi, r_lo = split2(ret[t])
        tile = jnp.concatenate([r_hi, r_lo, r_hi, ones], axis=0)
        rm[:, t * 128 : (t + 1) * 128] = tile.astype(BF16)
    last = jnp.where((row8 >= 3) & (row8 < 6), 1.0, 0.0)
    zero = jnp.zeros((8, 128), F32)
    rm[:, months * 128 : (months + 1) * 128] = jnp.concatenate(
        [zero, zero, zero, last], axis=0
    ).astype(BF16)

    first = sh[:, 0, :]
    paths = jnp.concatenate([first, first + sh[:, 1, :]], axis=0)
    spread = jnp.concatenate([paths] * RUN_Z, axis=1)
    lane16 = lax.broadcasted_iota(jnp.int32, (16, 128), 1)
    p1s[...] = jnp.where(lax.div(lane16, 128 // RUN_Z) == zl, spread, 0.0)

    def to_proj(src, dst, s, r, p):
        return pltpu.make_async_remote_copy(
            src_ref=src, dst_ref=dst, send_sem=s, recv_sem=r,
            device_id={"proj": p}, device_id_type=MESH,
        )

    def to_scen(src, dst, s, r, p):
        return pltpu.make_async_remote_copy(
            src_ref=src, dst_ref=dst, send_sem=s, recv_sem=r,
            device_id={"scen": p}, device_id_type=MESH,
        )

    step = 128
    for i in range(blocks):
        for c in copies_in(i):
            c.wait()
        for j in range(size // step):
            at = pl.ds(i * size + j * step, step)
            left = lm[at, :]
            f, b = fund_o[at, :], base_o[at, :]
            for t in range(0, months, 2):
                growth = matmul(left, rm[:, t * 128 : (t + 2) * 128])
                f = f * growth[:, :128]
                b = jnp.maximum(b, f)
                f = f * growth[:, 128:]
                b = jnp.maximum(b, f)
            scale = matmul(left, rm[:, months * 128 : (months + 1) * 128])
            f, b = f * scale, b * scale
            s = 1.0 - lb[at, :] / 12.0
            s2 = s * s
            s4 = s2 * s2
            n = force_o[at, :] * (s4 * s4 * s4)
            fund_o[at, :], base_o[at, :], force_o[at, :] = f, b, n
            w_hi, w_lo = split2(n * f)
            wsv[at, 0:128], wsv[at, 128:256] = w_hi.astype(BF16), w_lo.astype(BF16)
            s_hi, s_lo = split2(n * b)
            ssv[at, 0:128], ssv[at, 128:256] = s_hi.astype(BF16), s_lo.astype(BF16)

    l_sent, x_sent, a_sent = [[], []], [[], []], []
    for k in range(2):
        if k == 1:
            one_hots(1)
        got = matmul(hot[k, 0 : PLANE * SHARE, :], wsv[...])
        for b in range(PLANE):
            part = got[b * SHARE : (b + 1) * SHARE]
            sb[k, b, 0:SHARE, :] = part[:, :128] + part[:, 128:]
        got = matmul(hot[k, PLANE * SHARE :, :], ssv[...])
        for b in range(PLANE):
            part = got[b * BLOCK : (b + 1) * BLOCK]
            sb[k, b, SHARE:, :] = part[:, :128] + part[:, 128:]
        if k == 0:
            pl.semaphore_wait(barrier, 2 * PLANE - 1 + len(z_peers) + len(y_peers))
            a_sent = [
                to_scen(p1s, p1r.at[r], a_s.at[r], a_r.at[r], z_peers[r])
                for r in range(RUN_Z - 1)
            ]
            for c in a_sent:
                c.start()
        for src, dst, s, r, sent in ((sl, rl, l_s, l_r, l_sent), (sb, rb, x_s, x_r, x_sent)):
            for n in range(PLANE - 1):
                sent[k].append(
                    to_proj(
                        src.at[k, lax.rem(u + n + 1, PLANE)], dst.at[k, n],
                        s.at[k, n], r.at[k, n], peers[n],
                    )
                )
                sent[k][-1].start()

    for c in a_sent:
        c.wait_recv()
    p2s[...] = p1s[...] + p1r[0] + p1r[1] + p1r[2]
    y_sent = [
        to_scen(p2s, p2r.at[r], y_s.at[r], y_r.at[r], y_peers[r]) for r in range(RING_Y - 1)
    ]
    for c in y_sent:
        c.start()

    mix_pair = jnp.concatenate(split2(mix_norm), axis=0).astype(BF16)
    for k in range(2):
        for c in l_sent[k]:
            c.wait_recv()
        labs = [rl[k, n] for n in range(PLANE - 1)] + [sl[k, u]]
        lab = jnp.concatenate(
            [jnp.where(lane[0:2] < 64, labs[2 * i], labs[2 * i + 1]) for i in range(PLANE // 2)], axis=1
        )
        here, which = lab[0:1, :], lab[1:2, :]
        arrived_hot = jnp.where(
            lax.broadcasted_iota(jnp.int32, (products, PLANE * SHARE), 0).astype(F32) == which,
            1.0, 0.0,
        ).astype(BF16)
        pair = matmul(mix_pair, arrived_hot)
        m_hi, m_lo = pair[0:8], pair[8:16]

        def members(i, _):
            even = here == (2 * i).astype(F32)
            odd = here == (2 * i + 1).astype(F32)
            at = pl.ds(pl.multiple_of(i * 16, 16), 16)
            for ref, v in ((mh, m_hi), (ml, m_lo)):
                ref[k, at, :] = jnp.concatenate(
                    [jnp.where(even, v, 0.0), jnp.where(odd, v, 0.0)], axis=0
                ).astype(BF16)
            return 0

        lax.fori_loop(0, BLOCK // 2, members, 0, unroll=4)

    def partial(k, dst):
        for c in x_sent[k]:
            c.wait_recv()
        total = sb[k, u, SHARE:, :]
        for n in range(PLANE):
            mine = n == PLANE - 1
            hi, lo = split2(sb[k, u, 0:SHARE, :] if mine else rb[k, n, 0:SHARE, :])
            wmat[n * SHARE : (n + 1) * SHARE, 0:128] = hi.astype(BF16)
            wmat[n * SHARE : (n + 1) * SHARE, 128:256] = lo.astype(BF16)
            if not mine:
                total = total + rb[k, n, SHARE:, :]
        both = matmul(mh[k], wmat[...])
        sums = both[:, :128] + both[:, 128:] + matmul(ml[k], wmat[:, 0:128])
        for j in range(CHUNKS):
            dst[j, 0 : CHUNK * 8, :] = sums[j * CHUNK * 8 : (j + 1) * CHUNK * 8]
            dst[j, CHUNK * 8 :, :] = total[j * CHUNK : (j + 1) * CHUNK]

    partial(0, zs)
    z_sent = [
        to_proj(zs.at[j], zr.at[j], z_s.at[j], z_r.at[j], across) for j in range(CHUNKS)
    ]
    for c in z_sent:
        c.start()

    lapses = jnp.dot(
        table[...], prod_hot, precision=lax.Precision.HIGHEST, preferred_element_type=F32
    )
    picked = lax.broadcasted_iota(jnp.int32, lapses.shape, 0) == year[0]
    base_lapse = jnp.sum(jnp.where(picked, lapses, 0.0), axis=0, keepdims=True)
    cols = rows_of([coh_f, base_lapse], points).T
    brow[...] = jnp.broadcast_to(cols[:, 1:2], brow.shape)
    coh_col = cols[:, 0:1]
    for n in range(pick.shape[1] // 128):
        cohorts = (lax.broadcasted_iota(jnp.int32, (points, 128), 1) + n * 128).astype(F32)
        pick[:, n * 128 : (n + 1) * 128] = jnp.where(coh_col == cohorts, 1.0, 0.0).astype(BF16)

    for c in y_sent:
        c.wait_recv()
    for n in range(RING_Y):
        tile = p2s[...] if n == RING_Y - 1 else p2r[n]
        for k in range(2):
            hi, lo = split2(tile[k * 8 : (k + 1) * 8])
            years = jnp.where(row8 < 3, float(k + 1), 0.0)
            full = jnp.concatenate([hi, hi, lo, years], axis=0)
            at = (k * RING_Y + n) * 128
            lhs[at : at + 128, :] = full.T.astype(BF16)

    partial(1, own)

    trials = RING_Y * 128
    vols = rows_of([vol[f] for f in range(8)], 128)
    sig = sigma[...]
    level = sig * LOG2E
    drift = sig * sig * (-0.5 * LOG2E)
    c_sent = []
    for j in range(CHUNKS):
        z_sent[j].wait_recv()

        def price(i, _):
            tiles, money = [], []
            for e in range(2):
                c = i * 2 + e
                at = pl.ds(pl.multiple_of(c * 8, 8), 8)
                s = own[j, at, :] + zr[j, at, :]
                g = own[j, pl.ds(CHUNK * 8 + c, 1), :] + zr[j, pl.ds(CHUNK * 8 + c, 1), :]
                inv = 1.0 / jnp.sum(s, axis=0, keepdims=True)
                loads = s * inv * vols
                d = drift * jnp.sum(loads * loads, axis=0, keepdims=True)
                a_hi, a_lo = split2(loads * level)
                tiles.append(
                    jnp.concatenate([a_hi, a_lo, a_hi, rows_of(split3(d), 128)], axis=0)
                )
                money.append(g * inv)
            right = jnp.concatenate(tiles, axis=1).astype(BF16)
            strike = jnp.concatenate(money, axis=1)
            cost = jnp.zeros((1, 256), F32)
            for k in range(2):
                acc = jnp.zeros((8, 256), F32)
                for b in range(0, trials, 256):
                    at = k * trials + b
                    x = matmul(lhs[at : at + 256, :], right)
                    pay = jnp.maximum(strike - jnp.exp2(x), 0.0)
                    acc = acc + jnp.sum(pay.reshape(32, 8, 256), axis=0)
                cost = cost + jnp.sum(acc, axis=0, keepdims=True) * (0.96 ** (k + 1) / trials)
            factor = 0.3 + 2.0 / (1.0 + jnp.exp(5.0 * cost - 2.0))
            for e in range(2):
                at = pl.ds(j * CHUNK + i * 2 + e, 1)
                cost_o[at, :] = cost[:, e * 128 : (e + 1) * 128]
                lfv[at, :] = factor[:, e * 128 : (e + 1) * 128]
            return 0

        lax.fori_loop(0, CHUNK // 2, price, 0, unroll=2)
        for n, p in enumerate([*far, across, *peers]):
            c_sent.append(
                to_proj(
                    lfv.at[pl.ds(j * CHUNK, CHUNK)],
                    cb.at[pl.ds(pl.multiple_of(me * BLOCK + j * CHUNK, 8), CHUNK)],
                    c_s.at[j, n], c_r.at[j, n], p,
                )
            )
            c_sent[-1].start()

    cb[pl.ds(pl.multiple_of(me * BLOCK, 8), BLOCK), :] = lfv[...]
    for c in [*l_sent[0], *l_sent[1], *x_sent[0], *x_sent[1], *a_sent, *y_sent, *z_sent]:
        c.wait_send()
    for c in c_sent:
        c.wait_send()
    for c in c_sent:
        c.wait_recv()


def last_kernel(
    fund, force, base, pick, brow, cb, cost,
    fund_o, force_o, base_o, lapse_o, cost_o,
    out, sem, sem_out,
):
    outs = [
        pltpu.make_async_copy(src, dst, sem.at[n])
        for n, (src, dst) in enumerate(
            ((fund, fund_o), (force, force_o), (base, base_o), (cost, cost_o))
        )
    ]
    for c in outs:
        c.start()
    points = out.shape[0]
    factors = jnp.concatenate(split2(cb[...]), axis=1).astype(BF16)
    blocks = sem_out.shape[0]
    size = points // blocks
    for i in range(blocks):
        at = pl.ds(i * size, size)
        got = matmul(pick[at, :], factors)
        out[at, :] = (got[:, :128] + got[:, 128:]) * brow[at, :]
        outs.append(pltpu.make_async_copy(out.at[at], lapse_o.at[at], sem_out.at[i]))
        outs[-1].start()
    for c in outs:
        c.wait()


def body(
    fund_value, in_force, guarantee_base, lapse_rate, cohort, product, guarantee_type,
    returns, mix_table, fee_table, rollup_table, fund_vol, closing_sigma_figure, shocks,
    base_table, year_index,
):
    points, scens = fund_value.shape
    cohorts = BLOCK * lax.axis_size("proj")
    blocks = 4
    vmem = pl.BlockSpec(memory_space=pltpu.VMEM)
    hbm = pl.BlockSpec(memory_space=pl.ANY)
    dma = pltpu.SemaphoreType.DMA
    full = jax.ShapeDtypeStruct((points, scens), F32)
    own = jax.ShapeDtypeStruct((BLOCK, scens), F32)
    months = returns.shape[1]
    ints = pltpu.VMEM((1, points), jnp.int32)
    args = [
        fund_value, in_force, guarantee_base, lapse_rate,
        cohort.reshape(1, points), product.reshape(1, points), guarantee_type.reshape(1, points),
        returns.transpose(1, 0, 2), mix_table.T, base_table, shocks,
        closing_sigma_figure.reshape(1, scens), fee_table, rollup_table, fund_vol,
    ]
    args = [pltpu.with_memory_space_constraint(a, pltpu.HBM) for a in args]
    middle = pl.pallas_call(
        functools.partial(main_kernel, blocks),
        out_shape=(
            full, full, full,
            jax.ShapeDtypeStruct((points, cohorts), BF16),
            full,
            jax.ShapeDtypeStruct((cohorts, scens), F32),
            own,
        ),
        in_specs=[hbm] * 15 + [pl.BlockSpec(memory_space=pltpu.SMEM)],
        out_specs=(vmem,) * 7,
        scratch_shapes=[
            pltpu.VMEM((points, scens), F32),
            ints, ints, ints,
            pltpu.VMEM((months, 8, scens), F32),
            pltpu.VMEM((8, 16), F32),
            pltpu.VMEM(base_table.shape, F32),
            pltpu.VMEM(shocks.shape, F32),
            pltpu.VMEM((1, scens), F32),
            pltpu.SMEM(fee_table.shape, F32),
            pltpu.SMEM(rollup_table.shape, F32),
            pltpu.SMEM((8,), F32),
            pltpu.VMEM((points, KDIM), BF16),
            pltpu.VMEM((KDIM, (months + 1) * scens), BF16),
            *[pltpu.VMEM((points, 2 * scens), BF16)] * 2,
            pltpu.VMEM((2, PLANE * (SHARE + BLOCK), points), BF16),
            pltpu.VMEM((2, PLANE, 2, 128), F32),
            pltpu.VMEM((2, PLANE - 1, 2, 128), F32),
            pltpu.VMEM((2, PLANE, ROWS, scens), F32),
            pltpu.VMEM((2, PLANE - 1, ROWS, scens), F32),
            pltpu.VMEM((PLANE * SHARE, 2 * scens), BF16),
            *[pltpu.VMEM((2, BLOCK * 8, PLANE * SHARE), BF16)] * 2,
            *[pltpu.VMEM((CHUNKS, PART, scens), F32)] * 3,
            pltpu.VMEM((16, 128), F32),
            pltpu.VMEM((RUN_Z - 1, 16, 128), F32),
            pltpu.VMEM((16, 128), F32),
            pltpu.VMEM((RING_Y - 1, 16, 128), F32),
            pltpu.VMEM((2 * RING_Y * 128, KDIM), BF16),
            pltpu.VMEM((BLOCK, scens), F32),
            dma((11,)),
            dma((blocks, 4)),
            *[dma((2, PLANE - 1))] * 4,
            *[dma((CHUNKS,))] * 2,
            *[dma((RUN_Z - 1,))] * 2,
            *[dma((RING_Y - 1,))] * 2,
            *[dma((CHUNKS, 2 * PLANE - 1))] * 2,
        ],
        compiler_params=pltpu.CompilerParams(
            collective_id=0, has_side_effects=True, vmem_limit_bytes=28 << 20
        ),
    )(*args, year_index)
    return pl.pallas_call(
        last_kernel,
        out_shape=(full, full, full, full, own),
        in_specs=[vmem] * 7,
        out_specs=(hbm,) * 5,
        scratch_shapes=[pltpu.VMEM((points, scens), F32), dma((4,)), dma((4,))],
        compiler_params=pltpu.CompilerParams(vmem_limit_bytes=28 << 20),
    )(*middle)


def solution(mesh):
    wide, row, last = P("proj", "scen"), P("proj"), P(None, None, "scen")
    placed = (
        wide, wide, wide, wide, row, row, row, last,
        P(), P(), P(), P(), P("scen"), last, P(), P(),
    )
    return jax.shard_map(
        body, mesh=mesh, in_specs=placed, out_specs=(wide,) * 5, check_vma=False
    )
```

```python
import functools

import jax
import jax.numpy as jnp
from jax import lax
from jax.experimental import pallas as pl
from jax.experimental.pallas import tpu as pltpu
from jax.sharding import PartitionSpec as P

F32, BF16 = jnp.float32, jnp.bfloat16
MESH = pl.DeviceIdType.MESH
LOG2E = 1.4426950408889634

PLANES, PLANE = 2, 8
RING_Y, RUN_Z = 8, 4
SHARE, BLOCK = 64, 32
ROWS = SHARE + BLOCK
CHUNKS, CHUNK = 4, 8
PART = CHUNK * 8 + CHUNK
KDIM = 32


def split2(x):
    hi = x.astype(BF16).astype(F32)
    return hi, x - hi


def split3(x):
    hi, rest = split2(x)
    mid, lo = split2(rest)
    return hi, mid, lo


def matmul(a, b):
    return jnp.dot(a, b, preferred_element_type=F32)


def rows_of(pieces, lanes):
    row = lax.broadcasted_iota(jnp.int32, (8, lanes), 0)
    out = jnp.zeros((8, lanes), F32)
    for i, piece in enumerate(pieces):
        out = jnp.where(row == i, piece, out)
    return out


def main_kernel(
    blocks,
    fund, force, base, lapse, coh_h, prod_h, gtype_h, ret_h, mix_h, table_h, sh_h, sigma_h,
    fee_h, roll_h, vol_h, year,
    fund_o, force_o, base_o, pick, brow, cb, cost_o,
    lb, coh, prod, gtype, ret, mix, table, sh, sigma, fee, roll, vol,
    lm, rm, wsv, ssv, hot, sl, rl, sb, rb, wmat, mh, ml, zs, zr, own,
    p1s, p1r, p2s, p2r, lhs, lfv,
    sem_small, sem_in,
    l_s, l_r, x_s, x_r, z_s, z_r, a_s, a_r, y_s, y_r, c_s, c_r,
):
    points = lb.shape[0]
    size = points // blocks
    months = ret.shape[0]
    me, col = lax.axis_index("proj"), lax.axis_index("scen")
    h, u = lax.div(me, PLANE), lax.rem(me, PLANE)
    y, zl = lax.div(col, RUN_Z), lax.rem(col, RUN_Z)
    across = (1 - h) * PLANE + u
    x, core = lax.div(u, 2), lax.rem(u, 2)
    mates = [
        lax.rem(x + dx, PLANE // 2) * 2 + (1 - core if dc else core)
        for dx, dc in ((2, 0), (2, 1), (1, 0), (3, 0), (1, 1), (3, 1), (0, 1))
    ]
    peers = [h * PLANE + v for v in mates]
    far = [(1 - h) * PLANE + v for v in mates]
    z_peers = [y * RUN_Z + lax.rem(zl + r, RUN_Z) for r in range(1, RUN_Z)]
    y_peers = [lax.rem(y + r, RING_Y) * RUN_Z + zl for r in range(1, RING_Y)]

    smalls = [
        pltpu.make_async_copy(src, dst, sem_small.at[n])
        for n, (src, dst) in enumerate((
            (coh_h, coh), (prod_h, prod), (gtype_h, gtype), (mix_h, mix), (fee_h, fee),
            (roll_h, roll), (vol_h, vol), (ret_h, ret), (table_h, table),
            (sh_h, sh), (sigma_h, sigma),
        ))
    ]

    def copies_in(i):
        at = pl.ds(i * size, size)
        return [
            pltpu.make_async_copy(src.at[at], dst.at[at], sem_in.at[i, n])
            for n, (src, dst) in enumerate(
                ((fund, fund_o), (base, base_o), (force, force_o), (lapse, lb))
            )
        ]

    for c in smalls:
        c.start()
    for i in range(blocks):
        for c in copies_in(i):
            c.start()

    barrier = pltpu.get_barrier_semaphore()
    for p in [across, *peers]:
        pl.semaphore_signal(barrier, inc=1, device_id={"proj": p}, device_id_type=MESH)
    for p in [*z_peers, *y_peers]:
        pl.semaphore_signal(barrier, inc=1, device_id={"scen": p}, device_id_type=MESH)
    for c in smalls:
        c.wait()

    lane = lax.broadcasted_iota(jnp.int32, (8, 128), 1)
    row8 = lax.broadcasted_iota(jnp.int32, (8, 128), 0)

    owners = points // SHARE
    coh_row = coh[...]
    owner_row = lax.div(coh_row, BLOCK)
    owner_iota = lax.broadcasted_iota(jnp.int32, (owners, points), 0)
    owner_hot = jnp.where(owner_iota == owner_row, 1.0, 0.0)
    before = jnp.where(
        lax.broadcasted_iota(jnp.int32, (128, 128), 0)
        < lax.broadcasted_iota(jnp.int32, (128, 128), 1),
        1.0, 0.0,
    ).astype(BF16)
    offset = lax.broadcasted_iota(jnp.int32, (owners, 1), 0).astype(F32) * float(SHARE)
    places = []
    for b in range(points // 128):
        part = owner_hot[:, b * 128 : (b + 1) * 128]
        rank = matmul(part.astype(BF16), before) + offset
        places.append(jnp.sum(part * rank, axis=0, keepdims=True))
        offset = offset + jnp.sum(part, axis=1, keepdims=True)
    place = jnp.concatenate(places, axis=1)
    prod_row = prod[...]
    coh_f = coh_row.astype(F32)
    labels = rows_of(
        [(coh_row - owner_row * BLOCK).astype(F32), prod_row.astype(F32)], points
    ).astype(BF16)

    row16 = lax.broadcasted_iota(jnp.int32, (16, points), 0).astype(F32)
    nil = jnp.zeros((16, points), BF16)

    def tiled_hot(row):
        tile = jnp.floor(row * 0.0625)
        within = jnp.where(row16 == row - tile * 16.0, 1.0, 0.0).astype(BF16)
        return jnp.broadcast_to(tile, (16, points)).astype(BF16), within

    place_tile, place_hot = tiled_hot(place)
    coh_tile, coh_hot = tiled_hot(coh_f)

    def one_hots(k):
        plane = 1 - h if k == 0 else h

        def values(i, _):
            tile = (plane * (PLANE * SHARE // 16) + i).astype(F32).astype(BF16)
            hot[k, pl.ds(pl.multiple_of(i * 16, 16), 16), :] = jnp.where(
                place_tile == tile, place_hot, nil
            )
            return 0

        def sums(i, _):
            tile = (plane * (PLANE * BLOCK // 16) + i).astype(F32).astype(BF16)
            hot[k, pl.ds(pl.multiple_of(PLANE * SHARE + i * 16, 16), 16), :] = jnp.where(
                coh_tile == tile, coh_hot, nil
            )
            return 0

        lax.fori_loop(0, PLANE * SHARE // 16, values, 0, unroll=4)
        lax.fori_loop(0, PLANE * BLOCK // 16, sums, 0, unroll=4)
        lab = lax.dot_general(
            labels, hot[k, 0 : PLANE * SHARE, :], (((1,), (1,)), ((), ())),
            preferred_element_type=F32,
        )
        for i in range(PLANE // 2):
            x = lab[:, i * 128 : (i + 1) * 128]
            back = pltpu.roll(x, 64, 1)
            sl[k, 2 * i] = jnp.where(lane < 64, x, back)[0:2]
            sl[k, 2 * i + 1] = jnp.where(lane < 64, back, x)[0:2]

    one_hots(0)

    products = mix.shape[1]
    m = mix[...]
    mix_norm = m / jnp.sum(m, axis=0, keepdims=True)
    prod_hot = jnp.where(
        lax.broadcasted_iota(jnp.int32, (products, points), 0) == prod_row, 1.0, 0.0
    )
    mix_rows = jnp.dot(
        mix_norm, prod_hot, precision=lax.Precision.HIGHEST, preferred_element_type=F32
    )
    g = gtype[...]
    fee_row, roll_row = jnp.zeros(g.shape, F32), jnp.zeros(g.shape, F32)
    for k in range(fee.shape[0]):
        fee_row = jnp.where(g == k, fee[k], fee_row)
        roll_row = jnp.where(g == k, roll[k], roll_row)
    grow = 1.0 + roll_row / 12.0
    kappa = (1.0 - fee_row) / grow
    g2 = grow * grow
    g4 = g2 * g2
    grow_year = g4 * g4 * g4
    a_hi, a_lo = split2(mix_rows * kappa)
    extra = rows_of([*split3(kappa), *split3(grow_year)], points)
    left_rows = jnp.concatenate([a_hi, a_hi, a_lo, extra], axis=0)
    lm[...] = left_rows.T.astype(BF16)
    ones = jnp.where(row8 < 3, 1.0, 0.0)
    for t in range(months):
        r_hi, r_lo = split2(ret[t])
        tile = jnp.concatenate([r_hi, r_lo, r_hi, ones], axis=0)
        rm[:, t * 128 : (t + 1) * 128] = tile.astype(BF16)
    last = jnp.where((row8 >= 3) & (row8 < 6), 1.0, 0.0)
    zero = jnp.zeros((8, 128), F32)
    rm[:, months * 128 : (months + 1) * 128] = jnp.concatenate(
        [zero, zero, zero, last], axis=0
    ).astype(BF16)

    first = sh[:, 0, :]
    paths = jnp.concatenate([first, first + sh[:, 1, :]], axis=0)
    spread = jnp.concatenate([paths] * RUN_Z, axis=1)
    lane16 = lax.broadcasted_iota(jnp.int32, (16, 128), 1)
    p1s[...] = jnp.where(lax.div(lane16, 128 // RUN_Z) == zl, spread, 0.0)

    def to_proj(src, dst, s, r, p):
        return pltpu.make_async_remote_copy(
            src_ref=src, dst_ref=dst, send_sem=s, recv_sem=r,
            device_id={"proj": p}, device_id_type=MESH,
        )

    def to_scen(src, dst, s, r, p):
        return pltpu.make_async_remote_copy(
            src_ref=src, dst_ref=dst, send_sem=s, recv_sem=r,
            device_id={"scen": p}, device_id_type=MESH,
        )

    step = 128
    for i in range(blocks):
        for c in copies_in(i):
            c.wait()
        for j in range(size // step):
            at = pl.ds(i * size + j * step, step)
            left = lm[at, :]
            f, b = fund_o[at, :], base_o[at, :]
            for t in range(0, months, 2):
                growth = matmul(left, rm[:, t * 128 : (t + 2) * 128])
                f = f * growth[:, :128]
                b = jnp.maximum(b, f)
                f = f * growth[:, 128:]
                b = jnp.maximum(b, f)
            scale = matmul(left, rm[:, months * 128 : (months + 1) * 128])
            f, b = f * scale, b * scale
            s = 1.0 - lb[at, :] / 12.0
            s2 = s * s
            s4 = s2 * s2
            n = force_o[at, :] * (s4 * s4 * s4)
            fund_o[at, :], base_o[at, :], force_o[at, :] = f, b, n
            w_hi, w_lo = split2(n * f)
            wsv[at, 0:128], wsv[at, 128:256] = w_hi.astype(BF16), w_lo.astype(BF16)
            s_hi, s_lo = split2(n * b)
            ssv[at, 0:128], ssv[at, 128:256] = s_hi.astype(BF16), s_lo.astype(BF16)

    l_sent, x_sent, a_sent = [[], []], [[], []], []
    for k in range(2):
        if k == 1:
            one_hots(1)
        got = matmul(hot[k, 0 : PLANE * SHARE, :], wsv[...])
        for b in range(PLANE):
            part = got[b * SHARE : (b + 1) * SHARE]
            sb[k, b, 0:SHARE, :] = part[:, :128] + part[:, 128:]
        got = matmul(hot[k, PLANE * SHARE :, :], ssv[...])
        for b in range(PLANE):
            part = got[b * BLOCK : (b + 1) * BLOCK]
            sb[k, b, SHARE:, :] = part[:, :128] + part[:, 128:]
        if k == 0:
            pl.semaphore_wait(barrier, PLANE + len(z_peers) + len(y_peers))
            a_sent = [
                to_scen(p1s, p1r.at[r], a_s.at[r], a_r.at[r], z_peers[r])
                for r in range(RUN_Z - 1)
            ]
            for c in a_sent:
                c.start()
        for src, dst, s, r, sent in ((sl, rl, l_s, l_r, l_sent), (sb, rb, x_s, x_r, x_sent)):
            for n in range(PLANE - 1):
                sent[k].append(
                    to_proj(
                        src.at[k, mates[n]], dst.at[k, n],
                        s.at[k, n], r.at[k, n], peers[n],
                    )
                )
                sent[k][-1].start()

    for c in a_sent:
        c.wait_recv()
    p2s[...] = p1s[...] + p1r[0] + p1r[1] + p1r[2]
    y_sent = [
        to_scen(p2s, p2r.at[r], y_s.at[r], y_r.at[r], y_peers[r]) for r in range(RING_Y - 1)
    ]
    for c in y_sent:
        c.start()

    mix_pair = jnp.concatenate(split2(mix_norm), axis=0).astype(BF16)
    def select_rows(k):
        for c in l_sent[k]:
            c.wait_recv()
        labs = [rl[k, n] for n in range(PLANE - 1)] + [sl[k, u]]
        lab = jnp.concatenate(
            [jnp.where(lane[0:2] < 64, labs[2 * i], labs[2 * i + 1]) for i in range(PLANE // 2)], axis=1
        )
        here, which = lab[0:1, :], lab[1:2, :]
        arrived_hot = jnp.where(
            lax.broadcasted_iota(jnp.int32, (products, PLANE * SHARE), 0).astype(F32) == which,
            1.0, 0.0,
        ).astype(BF16)
        pair = matmul(mix_pair, arrived_hot)
        m_hi, m_lo = pair[0:8], pair[8:16]

        def members(i, _):
            even = here == (2 * i).astype(F32)
            odd = here == (2 * i + 1).astype(F32)
            at = pl.ds(pl.multiple_of(i * 16, 16), 16)
            for ref, v in ((mh, m_hi), (ml, m_lo)):
                ref[k, at, :] = jnp.concatenate(
                    [jnp.where(even, v, 0.0), jnp.where(odd, v, 0.0)], axis=0
                ).astype(BF16)
            return 0

        lax.fori_loop(0, BLOCK // 2, members, 0, unroll=4)

    def partial(k, dst):
        for c in x_sent[k]:
            c.wait_recv()
        total = sb[k, u, SHARE:, :]
        for n in range(PLANE):
            mine = n == PLANE - 1
            hi, lo = split2(sb[k, u, 0:SHARE, :] if mine else rb[k, n, 0:SHARE, :])
            wmat[n * SHARE : (n + 1) * SHARE, 0:128] = hi.astype(BF16)
            wmat[n * SHARE : (n + 1) * SHARE, 128:256] = lo.astype(BF16)
            if not mine:
                total = total + rb[k, n, SHARE:, :]
        both = matmul(mh[k], wmat[...])
        sums = both[:, :128] + both[:, 128:] + matmul(ml[k], wmat[:, 0:128])
        for j in range(CHUNKS):
            dst[j, 0 : CHUNK * 8, :] = sums[j * CHUNK * 8 : (j + 1) * CHUNK * 8]
            dst[j, CHUNK * 8 :, :] = total[j * CHUNK : (j + 1) * CHUNK]

    select_rows(0)
    partial(0, zs)
    z_sent = [
        to_proj(zs.at[j], zr.at[j], z_s.at[j], z_r.at[j], across) for j in range(CHUNKS)
    ]
    for c in z_sent:
        c.start()

    select_rows(1)

    lapses = jnp.dot(
        table[...], prod_hot, precision=lax.Precision.HIGHEST, preferred_element_type=F32
    )
    picked = lax.broadcasted_iota(jnp.int32, lapses.shape, 0) == year[0]
    base_lapse = jnp.sum(jnp.where(picked, lapses, 0.0), axis=0, keepdims=True)
    cols = rows_of([coh_f, base_lapse], points).T
    brow[...] = jnp.broadcast_to(cols[:, 1:2], brow.shape)
    coh_col = cols[:, 0:1]
    for n in range(pick.shape[1] // 128):
        cohorts = (lax.broadcasted_iota(jnp.int32, (points, 128), 1) + n * 128).astype(F32)
        pick[:, n * 128 : (n + 1) * 128] = jnp.where(coh_col == cohorts, 1.0, 0.0).astype(BF16)

    for c in y_sent:
        c.wait_recv()
    for n in range(RING_Y):
        tile = p2s[...] if n == RING_Y - 1 else p2r[n]
        for k in range(2):
            hi, lo = split2(tile[k * 8 : (k + 1) * 8])
            years = jnp.where(row8 < 3, float(k + 1), 0.0)
            full = jnp.concatenate([hi, hi, lo, years], axis=0)
            at = (k * RING_Y + n) * 128
            lhs[at : at + 128, :] = full.T.astype(BF16)

    partial(1, own)

    trials = RING_Y * 128
    vols = rows_of([vol[f] for f in range(8)], 128)
    sig = sigma[...]
    level = sig * LOG2E
    drift = sig * sig * (-0.5 * LOG2E)
    c_sent = []
    for j in range(CHUNKS):
        z_sent[j].wait_recv()

        def price(i, _):
            tiles, money = [], []
            for e in range(2):
                c = i * 2 + e
                at = pl.ds(pl.multiple_of(c * 8, 8), 8)
                s = own[j, at, :] + zr[j, at, :]
                g = own[j, pl.ds(CHUNK * 8 + c, 1), :] + zr[j, pl.ds(CHUNK * 8 + c, 1), :]
                inv = 1.0 / jnp.sum(s, axis=0, keepdims=True)
                loads = s * inv * vols
                d = drift * jnp.sum(loads * loads, axis=0, keepdims=True)
                a_hi, a_lo = split2(loads * level)
                tiles.append(
                    jnp.concatenate([a_hi, a_lo, a_hi, rows_of(split3(d), 128)], axis=0)
                )
                money.append(g * inv)
            right = jnp.concatenate(tiles, axis=1).astype(BF16)
            strike = jnp.concatenate(money, axis=1)
            cost = jnp.zeros((1, 256), F32)
            for k in range(2):
                acc = jnp.zeros((8, 256), F32)
                for b in range(0, trials, 256):
                    at = k * trials + b
                    x = matmul(lhs[at : at + 256, :], right)
                    pay = jnp.maximum(strike - jnp.exp2(x), 0.0)
                    acc = acc + jnp.sum(pay.reshape(32, 8, 256), axis=0)
                cost = cost + jnp.sum(acc, axis=0, keepdims=True) * (0.96 ** (k + 1) / trials)
            factor = 0.3 + 2.0 / (1.0 + jnp.exp(5.0 * cost - 2.0))
            for e in range(2):
                at = pl.ds(j * CHUNK + i * 2 + e, 1)
                cost_o[at, :] = cost[:, e * 128 : (e + 1) * 128]
                lfv[at, :] = factor[:, e * 128 : (e + 1) * 128]
            return 0

        lax.fori_loop(0, CHUNK // 2, price, 0, unroll=2)
        for n, p in enumerate([*far, across, *peers]):
            c_sent.append(
                to_proj(
                    lfv.at[pl.ds(j * CHUNK, CHUNK)],
                    cb.at[pl.ds(pl.multiple_of(me * BLOCK + j * CHUNK, 8), CHUNK)],
                    c_s.at[j, n], c_r.at[j, n], p,
                )
            )
            c_sent[-1].start()

    cb[pl.ds(pl.multiple_of(me * BLOCK, 8), BLOCK), :] = lfv[...]
    for c in [*l_sent[0], *l_sent[1], *x_sent[0], *x_sent[1], *a_sent, *y_sent, *z_sent]:
        c.wait_send()
    for c in c_sent:
        c.wait_send()
    for c in c_sent:
        c.wait_recv()


def last_kernel(
    fund, force, base, pick, brow, cb, cost,
    fund_o, force_o, base_o, lapse_o, cost_o,
    out, sem, sem_out,
):
    outs = [
        pltpu.make_async_copy(src, dst, sem.at[n])
        for n, (src, dst) in enumerate(
            ((fund, fund_o), (force, force_o), (base, base_o), (cost, cost_o))
        )
    ]
    for c in outs:
        c.start()
    points = out.shape[0]
    factors = jnp.concatenate(split2(cb[...]), axis=1).astype(BF16)
    blocks = sem_out.shape[0]
    size = points // blocks
    for i in range(blocks):
        at = pl.ds(i * size, size)
        got = matmul(pick[at, :], factors)
        out[at, :] = (got[:, :128] + got[:, 128:]) * brow[at, :]
        outs.append(pltpu.make_async_copy(out.at[at], lapse_o.at[at], sem_out.at[i]))
        outs[-1].start()
    for c in outs:
        c.wait()


def body(
    fund_value, in_force, guarantee_base, lapse_rate, cohort, product, guarantee_type,
    returns, mix_table, fee_table, rollup_table, fund_vol, closing_sigma_figure, shocks,
    base_table, year_index,
):
    points, scens = fund_value.shape
    cohorts = BLOCK * lax.axis_size("proj")
    blocks = 4
    vmem = pl.BlockSpec(memory_space=pltpu.VMEM)
    hbm = pl.BlockSpec(memory_space=pl.ANY)
    dma = pltpu.SemaphoreType.DMA
    full = jax.ShapeDtypeStruct((points, scens), F32)
    own = jax.ShapeDtypeStruct((BLOCK, scens), F32)
    months = returns.shape[1]
    ints = pltpu.VMEM((1, points), jnp.int32)
    args = [
        fund_value, in_force, guarantee_base, lapse_rate,
        cohort.reshape(1, points), product.reshape(1, points), guarantee_type.reshape(1, points),
        returns.transpose(1, 0, 2), mix_table.T, base_table, shocks,
        closing_sigma_figure.reshape(1, scens), fee_table, rollup_table, fund_vol,
    ]
    args = [pltpu.with_memory_space_constraint(a, pltpu.HBM) for a in args]
    middle = pl.pallas_call(
        functools.partial(main_kernel, blocks),
        out_shape=(
            full, full, full,
            jax.ShapeDtypeStruct((points, cohorts), BF16),
            full,
            jax.ShapeDtypeStruct((cohorts, scens), F32),
            own,
        ),
        in_specs=[hbm] * 15 + [pl.BlockSpec(memory_space=pltpu.SMEM)],
        out_specs=(vmem,) * 7,
        scratch_shapes=[
            pltpu.VMEM((points, scens), F32),
            ints, ints, ints,
            pltpu.VMEM((months, 8, scens), F32),
            pltpu.VMEM((8, 16), F32),
            pltpu.VMEM(base_table.shape, F32),
            pltpu.VMEM(shocks.shape, F32),
            pltpu.VMEM((1, scens), F32),
            pltpu.SMEM(fee_table.shape, F32),
            pltpu.SMEM(rollup_table.shape, F32),
            pltpu.SMEM((8,), F32),
            pltpu.VMEM((points, KDIM), BF16),
            pltpu.VMEM((KDIM, (months + 1) * scens), BF16),
            *[pltpu.VMEM((points, 2 * scens), BF16)] * 2,
            pltpu.VMEM((2, PLANE * (SHARE + BLOCK), points), BF16),
            pltpu.VMEM((2, PLANE, 2, 128), F32),
            pltpu.VMEM((2, PLANE - 1, 2, 128), F32),
            pltpu.VMEM((2, PLANE, ROWS, scens), F32),
            pltpu.VMEM((2, PLANE - 1, ROWS, scens), F32),
            pltpu.VMEM((PLANE * SHARE, 2 * scens), BF16),
            *[pltpu.VMEM((2, BLOCK * 8, PLANE * SHARE), BF16)] * 2,
            *[pltpu.VMEM((CHUNKS, PART, scens), F32)] * 3,
            pltpu.VMEM((16, 128), F32),
            pltpu.VMEM((RUN_Z - 1, 16, 128), F32),
            pltpu.VMEM((16, 128), F32),
            pltpu.VMEM((RING_Y - 1, 16, 128), F32),
            pltpu.VMEM((2 * RING_Y * 128, KDIM), BF16),
            pltpu.VMEM((BLOCK, scens), F32),
            dma((11,)),
            dma((blocks, 4)),
            *[dma((2, PLANE - 1))] * 4,
            *[dma((CHUNKS,))] * 2,
            *[dma((RUN_Z - 1,))] * 2,
            *[dma((RING_Y - 1,))] * 2,
            *[dma((CHUNKS, 2 * PLANE - 1))] * 2,
        ],
        compiler_params=pltpu.CompilerParams(
            collective_id=0, has_side_effects=True, vmem_limit_bytes=28 << 20
        ),
    )(*args, year_index)
    return pl.pallas_call(
        last_kernel,
        out_shape=(full, full, full, full, own),
        in_specs=[vmem] * 7,
        out_specs=(hbm,) * 5,
        scratch_shapes=[pltpu.VMEM((points, scens), F32), dma((4,)), dma((4,))],
        compiler_params=pltpu.CompilerParams(vmem_limit_bytes=28 << 20),
    )(*middle)


def solution(mesh):
    wide, row, last = P("proj", "scen"), P("proj"), P(None, None, "scen")
    placed = (
        wide, wide, wide, wide, row, row, row, last,
        P(), P(), P(), P(), P("scen"), last, P(), P(),
    )
    return jax.shard_map(
        body, mesh=mesh, in_specs=placed, out_specs=(wide,) * 5, check_vma=False
    )
```

```python
import functools

import jax
import jax.numpy as jnp
from jax import lax
from jax.experimental import pallas as pl
from jax.experimental.pallas import tpu as pltpu
from jax.sharding import PartitionSpec as P

F32, BF16 = jnp.float32, jnp.bfloat16
MESH = pl.DeviceIdType.MESH
LOG2E = 1.4426950408889634

PLANES, PLANE = 2, 8
RING_Y, RUN_Z = 8, 4
SHARE, BLOCK = 64, 32
ROWS = SHARE + BLOCK
CHUNKS, CHUNK = 4, 8
PART = CHUNK * 8 + CHUNK
KDIM = 32


def split2(x):
    hi = x.astype(BF16).astype(F32)
    return hi, x - hi


def split3(x):
    hi, rest = split2(x)
    mid, lo = split2(rest)
    return hi, mid, lo


def matmul(a, b):
    return jnp.dot(a, b, preferred_element_type=F32)


def rows_of(pieces, lanes):
    row = lax.broadcasted_iota(jnp.int32, (8, lanes), 0)
    out = jnp.zeros((8, lanes), F32)
    for i, piece in enumerate(pieces):
        out = jnp.where(row == i, piece, out)
    return out


def main_kernel(
    blocks,
    fund, force, base, lapse, coh_h, prod_h, gtype_h, ret_h, mix_h, table_h, sh_h, sigma_h,
    fee_h, roll_h, vol_h, year,
    fund_o, force_o, base_o, pick, brow, cb, cost_o,
    lb, coh, prod, gtype, ret, mix, table, sh, sigma, fee, roll, vol,
    lm, rm, wsv, ssv, hot, sl, rl, sb, rb, wmat, mh, ml, zs, zr, own, zx,
    p1s, p1r, p2s, p2r, lhs, lfv,
    sem_small, sem_in,
    l_s, l_r, x_s, x_r, z_s, z_r, a_s, a_r, y_s, y_r, c_s, c_r, e_s, e_r,
):
    points = lb.shape[0]
    size = points // blocks
    months = ret.shape[0]
    me, col = lax.axis_index("proj"), lax.axis_index("scen")
    h, u = lax.div(me, PLANE), lax.rem(me, PLANE)
    y, zl = lax.div(col, RUN_Z), lax.rem(col, RUN_Z)
    across = (1 - h) * PLANE + u
    x, core = lax.div(u, 2), lax.rem(u, 2)
    mates = [
        lax.rem(x + dx, PLANE // 2) * 2 + (1 - core if dc else core)
        for dx, dc in ((2, 0), (2, 1), (1, 0), (3, 0), (1, 1), (3, 1), (0, 1))
    ]
    peers = [h * PLANE + v for v in mates]
    far = [(1 - h) * PLANE + v for v in mates]
    z_peers = [y * RUN_Z + lax.rem(zl + r, RUN_Z) for r in range(1, RUN_Z)]
    y_peers = [lax.rem(y + r, RING_Y) * RUN_Z + zl for r in range(1, RING_Y)]

    smalls = [
        pltpu.make_async_copy(src, dst, sem_small.at[n])
        for n, (src, dst) in enumerate((
            (coh_h, coh), (prod_h, prod), (gtype_h, gtype), (mix_h, mix), (fee_h, fee),
            (roll_h, roll), (vol_h, vol), (ret_h, ret), (table_h, table),
            (sh_h, sh), (sigma_h, sigma),
        ))
    ]

    def copies_in(i):
        at = pl.ds(i * size, size)
        return [
            pltpu.make_async_copy(src.at[at], dst.at[at], sem_in.at[i, n])
            for n, (src, dst) in enumerate(
                ((fund, fund_o), (base, base_o), (force, force_o), (lapse, lb))
            )
        ]

    for c in smalls:
        c.start()
    for i in range(blocks):
        for c in copies_in(i):
            c.start()

    barrier = pltpu.get_barrier_semaphore()
    for p in [across, *peers]:
        pl.semaphore_signal(barrier, inc=1, device_id={"proj": p}, device_id_type=MESH)
    for p in [*z_peers, *y_peers]:
        pl.semaphore_signal(barrier, inc=1, device_id={"scen": p}, device_id_type=MESH)
    for c in smalls:
        c.wait()

    lane = lax.broadcasted_iota(jnp.int32, (8, 128), 1)
    row8 = lax.broadcasted_iota(jnp.int32, (8, 128), 0)

    owners = points // SHARE
    coh_row = coh[...]
    owner_row = lax.div(coh_row, BLOCK)
    owner_iota = lax.broadcasted_iota(jnp.int32, (owners, points), 0)
    owner_hot = jnp.where(owner_iota == owner_row, 1.0, 0.0)
    before = jnp.where(
        lax.broadcasted_iota(jnp.int32, (128, 128), 0)
        < lax.broadcasted_iota(jnp.int32, (128, 128), 1),
        1.0, 0.0,
    ).astype(BF16)
    offset = lax.broadcasted_iota(jnp.int32, (owners, 1), 0).astype(F32) * float(SHARE)
    places = []
    for b in range(points // 128):
        part = owner_hot[:, b * 128 : (b + 1) * 128]
        rank = matmul(part.astype(BF16), before) + offset
        places.append(jnp.sum(part * rank, axis=0, keepdims=True))
        offset = offset + jnp.sum(part, axis=1, keepdims=True)
    place = jnp.concatenate(places, axis=1)
    prod_row = prod[...]
    coh_f = coh_row.astype(F32)
    labels = rows_of(
        [(coh_row - owner_row * BLOCK).astype(F32), prod_row.astype(F32)], points
    ).astype(BF16)

    row16 = lax.broadcasted_iota(jnp.int32, (16, points), 0).astype(F32)
    nil = jnp.zeros((16, points), BF16)

    def tiled_hot(row):
        tile = jnp.floor(row * 0.0625)
        within = jnp.where(row16 == row - tile * 16.0, 1.0, 0.0).astype(BF16)
        return jnp.broadcast_to(tile, (16, points)).astype(BF16), within

    place_tile, place_hot = tiled_hot(place)
    coh_tile, coh_hot = tiled_hot(coh_f)

    def one_hots(k):
        plane = 1 - h if k == 0 else h

        def values(i, _):
            tile = (plane * (PLANE * SHARE // 16) + i).astype(F32).astype(BF16)
            hot[k, pl.ds(pl.multiple_of(i * 16, 16), 16), :] = jnp.where(
                place_tile == tile, place_hot, nil
            )
            return 0

        def sums(i, _):
            tile = (plane * (PLANE * BLOCK // 16) + i).astype(F32).astype(BF16)
            hot[k, pl.ds(pl.multiple_of(PLANE * SHARE + i * 16, 16), 16), :] = jnp.where(
                coh_tile == tile, coh_hot, nil
            )
            return 0

        lax.fori_loop(0, PLANE * SHARE // 16, values, 0, unroll=4)
        lax.fori_loop(0, PLANE * BLOCK // 16, sums, 0, unroll=4)
        lab = lax.dot_general(
            labels, hot[k, 0 : PLANE * SHARE, :], (((1,), (1,)), ((), ())),
            preferred_element_type=F32,
        )
        for i in range(PLANE // 2):
            x = lab[:, i * 128 : (i + 1) * 128]
            back = pltpu.roll(x, 64, 1)
            sl[k, 2 * i] = jnp.where(lane < 64, x, back)[0:2]
            sl[k, 2 * i + 1] = jnp.where(lane < 64, back, x)[0:2]

    one_hots(0)

    products = mix.shape[1]
    m = mix[...]
    mix_norm = m / jnp.sum(m, axis=0, keepdims=True)
    prod_hot = jnp.where(
        lax.broadcasted_iota(jnp.int32, (products, points), 0) == prod_row, 1.0, 0.0
    )
    mix_rows = jnp.dot(
        mix_norm, prod_hot, precision=lax.Precision.HIGHEST, preferred_element_type=F32
    )
    g = gtype[...]
    fee_row, roll_row = jnp.zeros(g.shape, F32), jnp.zeros(g.shape, F32)
    for k in range(fee.shape[0]):
        fee_row = jnp.where(g == k, fee[k], fee_row)
        roll_row = jnp.where(g == k, roll[k], roll_row)
    grow = 1.0 + roll_row / 12.0
    kappa = (1.0 - fee_row) / grow
    g2 = grow * grow
    g4 = g2 * g2
    grow_year = g4 * g4 * g4
    a_hi, a_lo = split2(mix_rows * kappa)
    extra = rows_of([*split3(kappa), *split3(grow_year)], points)
    left_rows = jnp.concatenate([a_hi, a_hi, a_lo, extra], axis=0)
    lm[...] = left_rows.T.astype(BF16)
    ones = jnp.where(row8 < 3, 1.0, 0.0)
    for t in range(months):
        r_hi, r_lo = split2(ret[t])
        tile = jnp.concatenate([r_hi, r_lo, r_hi, ones], axis=0)
        rm[:, t * 128 : (t + 1) * 128] = tile.astype(BF16)
    last = jnp.where((row8 >= 3) & (row8 < 6), 1.0, 0.0)
    zero = jnp.zeros((8, 128), F32)
    rm[:, months * 128 : (months + 1) * 128] = jnp.concatenate(
        [zero, zero, zero, last], axis=0
    ).astype(BF16)

    first = sh[:, 0, :]
    paths = jnp.concatenate([first, first + sh[:, 1, :]], axis=0)
    spread = jnp.concatenate([paths] * RUN_Z, axis=1)
    lane16 = lax.broadcasted_iota(jnp.int32, (16, 128), 1)
    p1s[...] = jnp.where(lax.div(lane16, 128 // RUN_Z) == zl, spread, 0.0)

    def to_proj(src, dst, s, r, p):
        return pltpu.make_async_remote_copy(
            src_ref=src, dst_ref=dst, send_sem=s, recv_sem=r,
            device_id={"proj": p}, device_id_type=MESH,
        )

    def to_scen(src, dst, s, r, p):
        return pltpu.make_async_remote_copy(
            src_ref=src, dst_ref=dst, send_sem=s, recv_sem=r,
            device_id={"scen": p}, device_id_type=MESH,
        )

    step = 128
    for i in range(blocks):
        for c in copies_in(i):
            c.wait()
        for j in range(size // step):
            at = pl.ds(i * size + j * step, step)
            left = lm[at, :]
            f, b = fund_o[at, :], base_o[at, :]
            for t in range(0, months, 2):
                growth = matmul(left, rm[:, t * 128 : (t + 2) * 128])
                f = f * growth[:, :128]
                b = jnp.maximum(b, f)
                f = f * growth[:, 128:]
                b = jnp.maximum(b, f)
            scale = matmul(left, rm[:, months * 128 : (months + 1) * 128])
            f, b = f * scale, b * scale
            s = 1.0 - lb[at, :] / 12.0
            s2 = s * s
            s4 = s2 * s2
            n = force_o[at, :] * (s4 * s4 * s4)
            fund_o[at, :], base_o[at, :], force_o[at, :] = f, b, n
            w_hi, w_lo = split2(n * f)
            wsv[at, 0:128], wsv[at, 128:256] = w_hi.astype(BF16), w_lo.astype(BF16)
            s_hi, s_lo = split2(n * b)
            ssv[at, 0:128], ssv[at, 128:256] = s_hi.astype(BF16), s_lo.astype(BF16)

    l_sent, x_sent, a_sent = [[], []], [[], []], []
    for k in range(2):
        if k == 1:
            one_hots(1)
        got = matmul(hot[k, 0 : PLANE * SHARE, :], wsv[...])
        for b in range(PLANE):
            part = got[b * SHARE : (b + 1) * SHARE]
            sb[k, b, 0:SHARE, :] = part[:, :128] + part[:, 128:]
        got = matmul(hot[k, PLANE * SHARE :, :], ssv[...])
        for b in range(PLANE):
            part = got[b * BLOCK : (b + 1) * BLOCK]
            sb[k, b, SHARE:, :] = part[:, :128] + part[:, 128:]
        if k == 0:
            pl.semaphore_wait(barrier, PLANE + len(z_peers) + len(y_peers))
            a_sent = [
                to_scen(p1s, p1r.at[r], a_s.at[r], a_r.at[r], z_peers[r])
                for r in range(RUN_Z - 1)
            ]
            for c in a_sent:
                c.start()
        for src, dst, s, r, sent in ((sl, rl, l_s, l_r, l_sent), (sb, rb, x_s, x_r, x_sent)):
            for n in range(PLANE - 1):
                sent[k].append(
                    to_proj(
                        src.at[k, mates[n]], dst.at[k, n],
                        s.at[k, n], r.at[k, n], peers[n],
                    )
                )
                sent[k][-1].start()

    for c in a_sent:
        c.wait_recv()
    p2s[...] = p1s[...] + p1r[0] + p1r[1] + p1r[2]
    y_sent = [
        to_scen(p2s, p2r.at[r], y_s.at[r], y_r.at[r], y_peers[r]) for r in range(RING_Y - 1)
    ]
    for c in y_sent:
        c.start()

    mix_pair = jnp.concatenate(split2(mix_norm), axis=0).astype(BF16)
    def select_rows(k):
        for c in l_sent[k]:
            c.wait_recv()
        labs = [rl[k, n] for n in range(PLANE - 1)] + [sl[k, u]]
        lab = jnp.concatenate(
            [jnp.where(lane[0:2] < 64, labs[2 * i], labs[2 * i + 1]) for i in range(PLANE // 2)], axis=1
        )
        here, which = lab[0:1, :], lab[1:2, :]
        arrived_hot = jnp.where(
            lax.broadcasted_iota(jnp.int32, (products, PLANE * SHARE), 0).astype(F32) == which,
            1.0, 0.0,
        ).astype(BF16)
        pair = matmul(mix_pair, arrived_hot)
        m_hi, m_lo = pair[0:8], pair[8:16]

        def members(i, _):
            even = here == (2 * i).astype(F32)
            odd = here == (2 * i + 1).astype(F32)
            at = pl.ds(pl.multiple_of(i * 16, 16), 16)
            for ref, v in ((mh, m_hi), (ml, m_lo)):
                ref[k, at, :] = jnp.concatenate(
                    [jnp.where(even, v, 0.0), jnp.where(odd, v, 0.0)], axis=0
                ).astype(BF16)
            return 0

        lax.fori_loop(0, BLOCK // 2, members, 0, unroll=4)

    def partial(k, dst):
        for c in x_sent[k]:
            c.wait_recv()
        total = sb[k, u, SHARE:, :]
        for n in range(PLANE):
            mine = n == PLANE - 1
            hi, lo = split2(sb[k, u, 0:SHARE, :] if mine else rb[k, n, 0:SHARE, :])
            wmat[n * SHARE : (n + 1) * SHARE, 0:128] = hi.astype(BF16)
            wmat[n * SHARE : (n + 1) * SHARE, 128:256] = lo.astype(BF16)
            if not mine:
                total = total + rb[k, n, SHARE:, :]
        both = matmul(mh[k], wmat[...])
        sums = both[:, :128] + both[:, 128:] + matmul(ml[k], wmat[:, 0:128])
        for j in range(CHUNKS):
            dst[j, 0 : CHUNK * 8, :] = sums[j * CHUNK * 8 : (j + 1) * CHUNK * 8]
            dst[j, CHUNK * 8 :, :] = total[j * CHUNK : (j + 1) * CHUNK]

    select_rows(0)
    partial(0, zs)
    z_sent = [
        to_proj(zs.at[j], zr.at[j], z_s.at[j], z_r.at[j], across) for j in range(CHUNKS)
    ]
    for c in z_sent:
        c.start()

    select_rows(1)

    lapses = jnp.dot(
        table[...], prod_hot, precision=lax.Precision.HIGHEST, preferred_element_type=F32
    )
    picked = lax.broadcasted_iota(jnp.int32, lapses.shape, 0) == year[0]
    base_lapse = jnp.sum(jnp.where(picked, lapses, 0.0), axis=0, keepdims=True)
    cols = rows_of([coh_f, base_lapse], points).T
    brow[...] = jnp.broadcast_to(cols[:, 1:2], brow.shape)
    coh_col = cols[:, 0:1]
    for n in range(pick.shape[1] // 128):
        cohorts = (lax.broadcasted_iota(jnp.int32, (points, 128), 1) + n * 128).astype(F32)
        pick[:, n * 128 : (n + 1) * 128] = jnp.where(coh_col == cohorts, 1.0, 0.0).astype(BF16)

    for c in y_sent:
        c.wait_recv()
    for n in range(RING_Y):
        tile = p2s[...] if n == RING_Y - 1 else p2r[n]
        for k in range(2):
            hi, lo = split2(tile[k * 8 : (k + 1) * 8])
            years = jnp.where(row8 < 3, float(k + 1), 0.0)
            full = jnp.concatenate([hi, hi, lo, years], axis=0)
            at = (k * RING_Y + n) * 128
            lhs[at : at + 128, :] = full.T.astype(BF16)

    partial(1, own)
    e_sent = to_proj(own.at[CHUNKS - 1], zx, e_s.at[0], e_r.at[0], across)
    e_sent.start()

    trials = RING_Y * 128
    vols = rows_of([vol[f] for f in range(8)], 128)
    sig = sigma[...]
    level = sig * LOG2E
    drift = sig * sig * (-0.5 * LOG2E)
    c_sent = []
    for j in range(CHUNKS + 1):
        both = j == CHUNKS
        if both:
            e_sent.wait_recv()
            mine, other = zs.at[CHUNKS - 1], zx
        else:
            z_sent[j].wait_recv()
            mine, other = own.at[j], zr.at[j]

        def price(i, _):
            tiles, money = [], []
            for e in range(2):
                c = i * 2 + e
                at = pl.ds(pl.multiple_of(c * 8, 8), 8)
                s = mine[at, :] + other[at, :]
                g = mine[pl.ds(CHUNK * 8 + c, 1), :] + other[pl.ds(CHUNK * 8 + c, 1), :]
                inv = 1.0 / jnp.sum(s, axis=0, keepdims=True)
                loads = s * inv * vols
                d = drift * jnp.sum(loads * loads, axis=0, keepdims=True)
                a_hi, a_lo = split2(loads * level)
                tiles.append(
                    jnp.concatenate([a_hi, a_lo, a_hi, rows_of(split3(d), 128)], axis=0)
                )
                money.append(g * inv)
            right = jnp.concatenate(tiles, axis=1).astype(BF16)
            strike = jnp.concatenate(money, axis=1)
            cost = jnp.zeros((1, 256), F32)
            for k in range(2):
                acc = jnp.zeros((8, 256), F32)
                for b in range(0, trials, 256):
                    at = k * trials + b
                    x = matmul(lhs[at : at + 256, :], right)
                    pay = jnp.maximum(strike - jnp.exp2(x), 0.0)
                    acc = acc + jnp.sum(pay.reshape(32, 8, 256), axis=0)
                cost = cost + jnp.sum(acc, axis=0, keepdims=True) * (0.96 ** (k + 1) / trials)
            factor = 0.3 + 2.0 / (1.0 + jnp.exp(5.0 * cost - 2.0))
            for e in range(2):
                at = pl.ds(j * CHUNK + i * 2 + e, 1)
                lfv[at, :] = factor[:, e * 128 : (e + 1) * 128]
                if not both:
                    cost_o[at, :] = cost[:, e * 128 : (e + 1) * 128]
            return 0

        lax.fori_loop(0, CHUNK // 2, price, 0, unroll=2)
        targets = [*peers, *far, across] if j < CHUNKS - 1 else peers
        row = across * BLOCK + (j - 1) * CHUNK if both else me * BLOCK + j * CHUNK
        if j < CHUNKS - 1:
            order = [*range(PLANE - 1, 2 * PLANE - 1), *range(PLANE - 1)]
        else:
            order = range(PLANE - 1)
        for n in order:
            c_sent.append(
                to_proj(
                    lfv.at[pl.ds(j * CHUNK, CHUNK)],
                    cb.at[pl.ds(pl.multiple_of(row, 8), CHUNK)],
                    c_s.at[j, n], c_r.at[j, n], targets[n],
                )
            )
            c_sent[-1].start()

    cb[pl.ds(pl.multiple_of(me * BLOCK, 8), BLOCK), :] = lfv[0:BLOCK, :]
    cb[pl.ds(pl.multiple_of(across * BLOCK + BLOCK - CHUNK, 8), CHUNK), :] = lfv[BLOCK:, :]
    e_sent.wait_send()
    for c in [*l_sent[0], *l_sent[1], *x_sent[0], *x_sent[1], *a_sent, *y_sent, *z_sent]:
        c.wait_send()
    for c in c_sent:
        c.wait_send()
    for c in c_sent:
        c.wait_recv()


def last_kernel(
    fund, force, base, pick, brow, cb, cost,
    fund_o, force_o, base_o, lapse_o, cost_o,
    out, sem, sem_out,
):
    outs = [
        pltpu.make_async_copy(src, dst, sem.at[n])
        for n, (src, dst) in enumerate(
            ((fund, fund_o), (force, force_o), (base, base_o), (cost, cost_o))
        )
    ]
    for c in outs:
        c.start()
    points = out.shape[0]
    factors = jnp.concatenate(split2(cb[...]), axis=1).astype(BF16)
    blocks = sem_out.shape[0]
    size = points // blocks
    for i in range(blocks):
        at = pl.ds(i * size, size)
        got = matmul(pick[at, :], factors)
        out[at, :] = (got[:, :128] + got[:, 128:]) * brow[at, :]
        outs.append(pltpu.make_async_copy(out.at[at], lapse_o.at[at], sem_out.at[i]))
        outs[-1].start()
    for c in outs:
        c.wait()


def body(
    fund_value, in_force, guarantee_base, lapse_rate, cohort, product, guarantee_type,
    returns, mix_table, fee_table, rollup_table, fund_vol, closing_sigma_figure, shocks,
    base_table, year_index,
):
    points, scens = fund_value.shape
    cohorts = BLOCK * lax.axis_size("proj")
    blocks = 4
    vmem = pl.BlockSpec(memory_space=pltpu.VMEM)
    hbm = pl.BlockSpec(memory_space=pl.ANY)
    dma = pltpu.SemaphoreType.DMA
    full = jax.ShapeDtypeStruct((points, scens), F32)
    own = jax.ShapeDtypeStruct((BLOCK, scens), F32)
    months = returns.shape[1]
    ints = pltpu.VMEM((1, points), jnp.int32)
    args = [
        fund_value, in_force, guarantee_base, lapse_rate,
        cohort.reshape(1, points), product.reshape(1, points), guarantee_type.reshape(1, points),
        returns.transpose(1, 0, 2), mix_table.T, base_table, shocks,
        closing_sigma_figure.reshape(1, scens), fee_table, rollup_table, fund_vol,
    ]
    args = [pltpu.with_memory_space_constraint(a, pltpu.HBM) for a in args]
    middle = pl.pallas_call(
        functools.partial(main_kernel, blocks),
        out_shape=(
            full, full, full,
            jax.ShapeDtypeStruct((points, cohorts), BF16),
            full,
            jax.ShapeDtypeStruct((cohorts, scens), F32),
            own,
        ),
        in_specs=[hbm] * 15 + [pl.BlockSpec(memory_space=pltpu.SMEM)],
        out_specs=(vmem,) * 7,
        scratch_shapes=[
            pltpu.VMEM((points, scens), F32),
            ints, ints, ints,
            pltpu.VMEM((months, 8, scens), F32),
            pltpu.VMEM((8, 16), F32),
            pltpu.VMEM(base_table.shape, F32),
            pltpu.VMEM(shocks.shape, F32),
            pltpu.VMEM((1, scens), F32),
            pltpu.SMEM(fee_table.shape, F32),
            pltpu.SMEM(rollup_table.shape, F32),
            pltpu.SMEM((8,), F32),
            pltpu.VMEM((points, KDIM), BF16),
            pltpu.VMEM((KDIM, (months + 1) * scens), BF16),
            *[pltpu.VMEM((points, 2 * scens), BF16)] * 2,
            pltpu.VMEM((2, PLANE * (SHARE + BLOCK), points), BF16),
            pltpu.VMEM((2, PLANE, 2, 128), F32),
            pltpu.VMEM((2, PLANE - 1, 2, 128), F32),
            pltpu.VMEM((2, PLANE, ROWS, scens), F32),
            pltpu.VMEM((2, PLANE - 1, ROWS, scens), F32),
            pltpu.VMEM((PLANE * SHARE, 2 * scens), BF16),
            *[pltpu.VMEM((2, BLOCK * 8, PLANE * SHARE), BF16)] * 2,
            *[pltpu.VMEM((CHUNKS, PART, scens), F32)] * 3,
            pltpu.VMEM((PART, scens), F32),
            pltpu.VMEM((16, 128), F32),
            pltpu.VMEM((RUN_Z - 1, 16, 128), F32),
            pltpu.VMEM((16, 128), F32),
            pltpu.VMEM((RING_Y - 1, 16, 128), F32),
            pltpu.VMEM((2 * RING_Y * 128, KDIM), BF16),
            pltpu.VMEM((BLOCK + CHUNK, scens), F32),
            dma((11,)),
            dma((blocks, 4)),
            *[dma((2, PLANE - 1))] * 4,
            *[dma((CHUNKS,))] * 2,
            *[dma((RUN_Z - 1,))] * 2,
            *[dma((RING_Y - 1,))] * 2,
            *[dma((CHUNKS + 1, 2 * PLANE - 1))] * 2,
            *[dma((1,))] * 2,
        ],
        compiler_params=pltpu.CompilerParams(
            collective_id=0, has_side_effects=True, vmem_limit_bytes=28 << 20
        ),
    )(*args, year_index)
    return pl.pallas_call(
        last_kernel,
        out_shape=(full, full, full, full, own),
        in_specs=[vmem] * 7,
        out_specs=(hbm,) * 5,
        scratch_shapes=[pltpu.VMEM((points, scens), F32), dma((4,)), dma((4,))],
        compiler_params=pltpu.CompilerParams(vmem_limit_bytes=28 << 20),
    )(*middle)


def solution(mesh):
    wide, row, last = P("proj", "scen"), P("proj"), P(None, None, "scen")
    placed = (
        wide, wide, wide, wide, row, row, row, last,
        P(), P(), P(), P(), P("scen"), last, P(), P(),
    )
    return jax.shard_map(
        body, mesh=mesh, in_specs=placed, out_specs=(wide,) * 5, check_vma=False
    )
```
